256 devices in a mesh: blk: 32 (over x, z), pair: 8 (over y, core).
Axes of the slice: x: 4, y: 4, z: 8, core: 2. Of those that a mesh axis runs over, the one named last changes fastest.
Arguments:
- features: float32 [64, 262144], P(None, 'blk'), may hold values from -6 to 6
- inv_scale: float32 [64], replicated, may hold values from 0.03125 to 20
- signal: float32 [1], replicated, may hold values from 0.110485435 to 0.44194174
- noise_var: float32 [262144], P('blk'), may hold values from 0.5 to 2
- right_side: float32 [32, 262144], P(None, 'blk'), may hold values from -30 to 30
- block_pairs: int32 [512, 2], P(('blk', 'pair')), may hold values from -1 to 127, as said below
Outputs:
- solution: float32 [32, 262144], P(None, 'blk')
- residual: float32 [32, 262144], P(None, 'blk')
The draws below stay inside these ranges and needn't reach their ends.
Inputs may be any that keep to these rules, and one draw needn't show every extreme that they name: `block_pairs`: rows run over the blk index, then the pair index, then 2 slots of one device. In each device's slots the live pairs come first; dead slots hold -1 in both columns. A live pair (i, j) has block i among blocks blk index * 4 to blk index * 4 + 3 of the device's blk index, and j equal to i or i + 1. Every block's pair (i, i) is listed once and no pair twice. In each blk index some device has all its slots live.
All inputs are finite; a program needn't handle non-finite values.
Results may differ from the reference program's by a relative error of at most 0.0011.
Values sent between devices are 32-bit elements; how exact they have to be, the bound alone decides.
A program may use at most 64 MiB of HBM per device.

```python
import math
import jax
import jax.numpy as jnp
from jax import lax

BS = 2048
F = 64
R = 32
ITERS = 2
BLK_DEV = 4
PAIRS_DEV = 2
NOBS = 262144
N_BLK = 32
N_PAIR = 8


def draw_block_pairs(key, part):
    groups = N_BLK
    options = 2 * BLK_DEV
    coin_key, score_key, deal_key = jax.random.split(jax.random.fold_in(key, 11), 3)
    column = jnp.arange(options, dtype=jnp.int32)[None, :]
    group_ids = jnp.arange(groups, dtype=jnp.int32)[:, None]
    row_block = group_ids * BLK_DEV + column % BLK_DEV
    col_block = row_block + column // BLK_DEV
    allowed = col_block < BLK_DEV * N_BLK
    coin_flips = jax.random.randint(coin_key, (groups, options), 0, 5) < 3
    living = allowed & ((column < BLK_DEV) | coin_flips)
    scores = jax.random.randint(score_key, (groups, options), 0, 4096) * options + column
    keyed = jnp.where(living, scores, 8192 * options + column)
    ordering = jnp.argsort(keyed, axis=1, stable=True)
    counted = jnp.sum(living.astype(jnp.int32), axis=1)
    dealing = jax.vmap(lambda sub_key: jax.random.permutation(sub_key, N_PAIR))(jax.random.split(deal_key, groups))
    placing = jnp.argsort(dealing, axis=1)
    positions = placing[:, :, None] * PAIRS_DEV + jnp.arange(PAIRS_DEV, dtype=jnp.int32)[None, None, :]
    filled = positions < counted[:, None, None]
    flat_positions = jnp.minimum(positions, options - 1).reshape(groups, -1)
    picked = jnp.take_along_axis(ordering, flat_positions, axis=1)
    row_pick = jnp.take_along_axis(jnp.broadcast_to(row_block, (groups, options)), picked, axis=1).reshape(filled.shape)
    col_pick = jnp.take_along_axis(jnp.broadcast_to(col_block, (groups, options)), picked, axis=1).reshape(filled.shape)
    result = jnp.stack([jnp.where(filled, row_pick, -1), jnp.where(filled, col_pick, -1)], axis=-1)
    return result.reshape(groups * N_PAIR * PAIRS_DEV, 2).astype(jnp.int32)


def draw_inv_scale(key, part):
    small_key, large_key, pick_key = jax.random.split(jax.random.fold_in(key, 37), 3)
    highest = 5 * F // 16 * 1.0
    lowest_large = 0.6 * highest
    smallest = 2.0 ** (-5)
    largest_small = 0.5
    order = jax.random.permutation(pick_key, F)
    picked_large = order < 2
    small_values = jnp.exp(jax.random.uniform(small_key, (F,), minval=jnp.log(smallest), maxval=jnp.log(largest_small)))
    large_values = jnp.exp(jax.random.uniform(large_key, (F,), minval=jnp.log(lowest_large), maxval=jnp.log(highest)))
    values = jnp.where(picked_large, large_values, small_values)
    return jnp.clip(values, smallest, highest).astype(jnp.float32)


def draw_right_side(key, part):
    base_key = jax.random.fold_in(jax.random.fold_in(key, 23), 0)
    columns = NOBS
    rising = jnp.sqrt(1.0 + 2.0 * jnp.arange(columns, dtype=jnp.float32) / columns)
    values = jax.random.normal(base_key, (R, columns))
    return jnp.clip(values * rising[None, :], -30.0, 30.0).astype(jnp.float32)


def steps_of(stream_key, dims, shards, low, high):
    gain, own = 1.0, jax.random.fold_in(stream_key, 6)
    for axis_at, shards_of in shards:
        heights = jnp.exp(jax.random.uniform(jax.random.fold_in(own, axis_at), (shards_of,), jnp.float32, low / len(shards), high / len(shards)))
        gain = gain * jnp.repeat(heights, dims[axis_at] // shards_of).reshape([-1 if axis == axis_at else 1 for axis in range(len(dims))])
    return gain


def scatter_about(rng, dims, scale, bound, shards=(), held_as=jnp.bfloat16):
    entries = scale * jax.random.normal(rng, dims, jnp.float32)
    if shards:
        entries = entries * steps_of(rng, dims, shards, -0.22, 0.18)
    return jnp.clip(entries, -bound, bound).astype(held_as)


def setup_inputs(seed: int = 0) -> dict:
    keys = jax.random.split(jax.random.key(seed), 7)
    features = scatter_about(keys[0], (F, NOBS), 1.0, 6.0, ((1, 32),), jnp.float32)
    inv_scale = draw_inv_scale(jax.random.fold_in(keys[6], 71), 0)
    signal = jnp.clip(jnp.exp(jax.random.uniform(keys[2], (1,), jnp.float32, math.log(0.110485435), math.log(0.44194174))), 0.110485435, 0.44194174)
    noise_var = jnp.clip(jnp.exp(math.log(2.0) - 1.3862944 * jax.random.uniform(keys[3], (NOBS,), jnp.float32) ** steps_of(keys[3], (NOBS,), ((0, 32),), -0.2, 0.2)), 0.5, 2.0)
    right_side = draw_right_side(jax.random.fold_in(keys[6], 71), 0)
    block_pairs = draw_block_pairs(jax.random.fold_in(keys[6], 71), 0)
    return dict(features=features, inv_scale=inv_scale, signal=signal, noise_var=noise_var, right_side=right_side, block_pairs=block_pairs)


root_three = 1.7320508075688772
taper_radius = 2.0

def kernel_tile(left_scaled, right_scaled, amplitude):
    cross = lax.dot_general(left_scaled, right_scaled, (((0,), (0,)), ((), ())), precision=lax.Precision.HIGHEST, preferred_element_type=jnp.float32)
    left_norms = lax.optimization_barrier(jnp.sum(left_scaled * left_scaled, axis=0))
    right_norms = lax.optimization_barrier(jnp.sum(right_scaled * right_scaled, axis=0))
    squared = (left_norms[:, None] + right_norms[None, :] - 2.0 * cross) / left_scaled.shape[0]
    distance = jnp.sqrt(jnp.maximum(squared, 0.0))
    stretched = root_three * distance
    ratio = distance / taper_radius
    taper = jnp.maximum(1.0 - ratio, 0.0) ** 4 * (1.0 + 4.0 * ratio)
    return amplitude * (1.0 + stretched) * jnp.exp(-stretched) * taper

def apply_operator(direction, scaled, block_pairs, amplitude, noise_var):
    halved = direction.astype(jnp.bfloat16)

    def visit(summed, listed):
        row_block = listed[0].astype(jnp.int32)
        col_block = listed[1].astype(jnp.int32)

        def work(summed):
            row_start = (row_block * BS).astype(jnp.int32)
            col_start = (col_block * BS).astype(jnp.int32)
            kernel_block = kernel_tile(lax.dynamic_slice_in_dim(scaled, row_start, BS, 1), lax.dynamic_slice_in_dim(scaled, col_start, BS, 1), amplitude)
            block_half = kernel_block.astype(jnp.bfloat16)
            crossing = (row_block != col_block).astype(jnp.float32)
            left_dir = lax.dynamic_slice_in_dim(direction, row_start, BS, 1)
            right_dir = lax.dynamic_slice_in_dim(direction, col_start, BS, 1)
            left_half = lax.dynamic_slice_in_dim(halved, row_start, BS, 1)
            right_half = lax.dynamic_slice_in_dim(halved, col_start, BS, 1)
            term_left = lax.dot_general(right_half, block_half, (((1,), (1,)), ((), ())), preferred_element_type=jnp.float32) + crossing * lax.optimization_barrier(jnp.sum(kernel_block, axis=1))[None, :] * left_dir
            term_right = crossing * (jnp.dot(left_half, block_half, preferred_element_type=jnp.float32) + lax.optimization_barrier(jnp.sum(kernel_block, axis=0))[None, :] * right_dir)
            summed = lax.dynamic_update_slice_in_dim(summed, lax.dynamic_slice_in_dim(summed, row_start, BS, 1) + term_left, row_start, 1)
            summed = lax.dynamic_update_slice_in_dim(summed, lax.dynamic_slice_in_dim(summed, col_start, BS, 1) + term_right, col_start, 1)
            return summed
        return (lax.cond(row_block >= 0, work, lambda unchanged: unchanged, summed), None)
    summed, _ = lax.scan(visit, jnp.zeros(direction.shape, jnp.float32), block_pairs)
    return noise_var[None, :] * direction + summed

def reference(features, inv_scale, signal, noise_var, right_side, block_pairs):
    scaled = features * inv_scale[:, None]
    amplitude = signal[0]
    solution = jnp.zeros_like(right_side)
    residual = right_side
    direction = right_side
    norm_now = lax.optimization_barrier(jnp.sum(residual * residual, axis=1))
    for iteration in range(ITERS):
        applied = apply_operator(direction, scaled, block_pairs, amplitude, noise_var)
        step_size = norm_now / lax.optimization_barrier(jnp.sum(direction * applied, axis=1))
        solution = solution + step_size[:, None] * direction
        residual = residual - step_size[:, None] * applied
        if iteration + 1 < ITERS:
            norm_next = lax.optimization_barrier(jnp.sum(residual * residual, axis=1))
            direction = residual + (norm_next / norm_now)[:, None] * direction
            norm_now = norm_next
    return (solution, residual)
```

```python
import functools
import math

import jax
import jax.numpy as jnp
from jax import lax
from jax.experimental import pallas as pl
from jax.experimental.pallas import tpu as pltpu
from jax.sharding import PartitionSpec as P

F = 64
R = 32
CHIPS = 4
TORUS = {32: (4, 8), 8: (2, 4), 2: (1, 2)}
LANES = 256
TERMS = 512
MESH = pl.DeviceIdType.MESH

ROOT3 = math.sqrt(3.0)
W = 2.0 * ROOT3 * math.log2(math.e)
SCALE = 2.0**-W / W**4
Q0 = 5.0 * (1.0 + 2.0 * ROOT3) * SCALE
Q1 = -(4.0 * (1.0 + 2.0 * ROOT3) + 10.0 * ROOT3) / W * SCALE
Q2 = 8.0 * ROOT3 / W**2 * SCALE
TINY = 1e-30


def split3(s):
    hi = s.astype(jnp.bfloat16)
    rest = s - hi.astype(jnp.float32)
    mid = rest.astype(jnp.bfloat16)
    lo = (rest - mid.astype(jnp.float32)).astype(jnp.bfloat16)
    return hi, mid, lo


def norm_rows(norms, first):
    n = norms.shape[1]
    hi, mid, lo = split3(norms)
    row = lax.broadcasted_iota(jnp.int32, (8, n), 0)
    base = 0 if first else 3
    ones = (row >= 3 - base) & (row < 6 - base)
    top = jnp.where(row == base, hi.astype(jnp.float32), 0.0)
    top = jnp.where(row == base + 1, mid.astype(jnp.float32), top)
    top = jnp.where(row == base + 2, lo.astype(jnp.float32), top)
    top = jnp.where(ones, 1.0, top)
    return jnp.concatenate([top, jnp.zeros((F - 8, n), jnp.float32)], 0).astype(jnp.bfloat16)


def left_terms(x, inv):
    s = x * inv
    norms = jnp.sum(s * s, axis=0, keepdims=True)
    hi, mid, lo = split3(-2.0 * s)
    return jnp.concatenate([hi, mid], 0).T, jnp.concatenate([lo, norm_rows(norms, False)], 0).T


def right_terms(x, inv):
    s = x * inv
    norms = jnp.sum(s * s, axis=0, keepdims=True)
    hi, mid, lo = split3(s)
    return jnp.concatenate([hi, hi, mid, mid, lo, jnp.zeros_like(lo), hi, norm_rows(norms, True)], 0)


def tile_values(sq, c0, c1, c2):
    y = jnp.maximum(sq, TINY)
    w = y * lax.rsqrt(y)
    u = jnp.maximum(W - w, 0.0)
    u2 = u * u
    return ((c2 * u + c1) * u + c0) * jnp.exp2(u) * (u2 * u2)


def tile_pass(slot, ch, bs, l_ref, r_ref, k_ref, v_ref, p_ref, s_ref, sig, sq_ref, h_ref):
    c0, c1, c2 = sig * Q0, sig * Q1, sig * Q2
    n = bs // ch
    base = slot * bs

    def lanes(j, _):
        cols = pl.ds(pl.multiple_of(j * LANES, LANES), LANES)

        def at(i):
            return pl.ds(pl.multiple_of(base + i * ch, ch), ch)

        def cross(i, buf):
            sq_ref[buf] = jnp.dot(l_ref[at(i), :], r_ref[:, cols], preferred_element_type=jnp.float32)

        def values(i, buf, sums):
            t = tile_values(sq_ref[buf], c0, c1, c2)
            half = t.astype(jnp.bfloat16)
            h_ref[buf] = half
            k_ref[at(i), cols] = half
            return sums + jnp.sum(t.reshape(ch // 8, 8, LANES), axis=0)

        def prod(i, buf, acc):
            return acc + jnp.dot(v_ref[:, at(i)], h_ref[buf], preferred_element_type=jnp.float32)

        acc = jnp.zeros((R, LANES), jnp.float32)
        sums = jnp.zeros((8, LANES), jnp.float32)
        cross(0, 0)
        cross(1, 1)
        sums = values(0, 0, sums)

        def rows(m, carry):
            acc, sums = carry
            i = 2 * m + 1
            cross(i + 1, 0)
            sums = values(i, 1, sums)
            acc = prod(i - 1, 0, acc)
            cross(i + 2, 1)
            sums = values(i + 1, 0, sums)
            acc = prod(i, 1, acc)
            return acc, sums

        acc, sums = lax.fori_loop(0, (n - 2) // 2, rows, (acc, sums))
        sums = values(n - 1, 1, sums)
        acc = prod(n - 2, 0, acc)
        acc = prod(n - 1, 1, acc)
        p_ref[slot, :, cols] = acc
        s_ref[slot, :, cols] = jnp.broadcast_to(jnp.sum(sums, axis=0, keepdims=True), (8, LANES))
        return 0

    lax.fori_loop(0, p_ref.shape[2] // LANES, lanes, 0)


def kernel(
    nx, nz, bs,
    x_hbm, inv_ref, sig_ref, noise_hbm, b_hbm, pairs_ref,
    sol_hbm, res_hbm,
    x_ref, l_ref, r_ref, k_ref, b_ref, bh_ref, q1_ref, qh_ref, q2_ref, v_ref,
    p_ref, s_ref, noise_ref, sq_ref, h_ref, flag_ref, group_ref, st_ref, sx_ref, sz_ref,
    sol_ref, res_ref,
    local_sem, out_sem, halo_send, halo_recv, flag_send, flag_recv, sum_send, sum_recv, part_send, part_recv,
):
    own = bs // 2
    ch = bs // 4
    count = nx * nz
    g = lax.axis_index("blk")
    me = lax.axis_index("pair")
    y, h = me // 2, me % 2
    gx, gz = g // nz, g % nz
    up, down, across = (y + 1) % CHIPS, (y + CHIPS - 1) % CHIPS, (y + 2) % CHIPS
    partner = (g, y * 2 + 1 - h)
    after, before = (g + 1) % count, (g + count - 1) % count
    edge = (y == 0) | (y == CHIPS - 1)
    first = jnp.where(y == 0, 1, y - 1)
    last = jnp.minimum(y + 1, CHIPS - 1)

    def block(i):
        return pl.ds(pl.multiple_of(i * bs, bs), bs)

    def piece(i):
        return pl.ds(pl.multiple_of(i * own, own), own)

    mine = piece(me)

    barrier = pltpu.get_barrier_semaphore()

    def greet(device):
        pl.semaphore_signal(barrier, inc=1, device_id=device, device_id_type=MESH)

    for k in range(1, 8):
        greet((g, (me + k) % 8))
    for k in range(1, nx):
        greet((((gx + k) % nx) * nz + gz, me))
    for k in range(1, nz):
        greet((gx * nz + (gz + k) % nz, me))

    @pl.when(y == CHIPS - 1)
    def _():
        greet((after, h))

    @pl.when(y == 0)
    def _():
        greet((before, (CHIPS - 1) * 2 + h))

    load_x0 = pltpu.make_async_copy(x_hbm.at[:, block(y)], x_ref.at[:, pl.ds(0, bs)], local_sem.at[0])
    load_x1 = pltpu.make_async_copy(x_hbm.at[:, block(first)], x_ref.at[:, pl.ds(bs, bs)], local_sem.at[1])
    load_x2 = pltpu.make_async_copy(x_hbm.at[:, block(last)], x_ref.at[:, pl.ds(2 * bs, bs)], local_sem.at[2])
    load_b = pltpu.make_async_copy(b_hbm, b_ref, local_sem.at[3])
    load_bh = pltpu.make_async_copy(b_hbm.at[:, block(last)], bh_ref, local_sem.at[4])
    load_noise = pltpu.make_async_copy(noise_hbm.at[:, mine], noise_ref, local_sem.at[5])
    load_x0.start()
    load_b.start()
    load_x1.start()
    load_noise.start()

    @pl.when(jnp.logical_not(edge))
    def _():
        load_x2.start()
        load_bh.start()

    row = lax.broadcasted_iota(jnp.int32, (8, 128), 0)
    flags = jnp.zeros((8, 128), jnp.float32)
    for k in range(CHIPS):
        left = g * CHIPS + k
        listed = jnp.float32(0.0)
        for s in range(2):
            hit = (pairs_ref[s, 0] == left) & (pairs_ref[s, 1] == left + 1)
            listed = listed + jnp.where(hit, 1.0, 0.0)
        flags = jnp.where(row == k, listed, flags)
    flag_ref[me] = flags

    inv = jnp.tile(inv_ref[...], (1, ch // 128))

    def prepare(slot):
        def part(i, _):
            at = pl.ds(pl.multiple_of(slot * bs + i * ch, ch), ch)
            a, c = left_terms(x_ref[:, at], inv)
            l_ref[at, 0:128] = a
            l_ref[at, 128:256] = a
            l_ref[at, 256:384] = a
            l_ref[at, 384:512] = c
            return 0

        lax.fori_loop(0, bs // ch, part, 0)

    load_x0.wait()
    prepare(0)
    for i in range(own // ch):
        at = pl.ds(pl.multiple_of(h * own + i * ch, ch), ch)
        r_ref[:, i * ch : (i + 1) * ch] = right_terms(x_ref[:, at], inv)
    load_b.wait()
    v_ref[:, 0:bs] = b_ref[:, block(y)].astype(jnp.bfloat16)

    pl.semaphore_wait(barrier, 5 + nx + nz + jnp.where(edge, 1, 0))

    half = pl.ds(pl.multiple_of(h * own, own), own)
    half_x = pl.ds(pl.multiple_of(2 * bs + h * own, own), own)
    other = pl.ds(pl.multiple_of((1 - h) * own, own), own)
    other_x = pl.ds(pl.multiple_of(2 * bs + (1 - h) * own, own), own)

    def halo_x(device, src):
        return pltpu.make_async_remote_copy(
            x_hbm.at[:, piece(src)], x_ref.at[:, half_x], halo_send.at[0], halo_recv.at[h],
            device_id=device, device_id_type=MESH)

    def halo_b(device, src):
        return pltpu.make_async_remote_copy(
            b_hbm.at[:, piece(src)], bh_ref.at[:, half], halo_send.at[1], halo_recv.at[2 + h],
            device_id=device, device_id_type=MESH)

    def halo_q(device):
        return pltpu.make_async_remote_copy(
            q1_ref.at[:, mine], qh_ref.at[:, half], halo_send.at[2], halo_recv.at[4 + h],
            device_id=device, device_id_type=MESH)

    def pass_on(ref, at, k, sem):
        return pltpu.make_async_remote_copy(
            ref.at[:, at], ref.at[:, at], halo_send.at[3 + k], halo_recv.at[2 * k + sem],
            device_id=partner, device_id_type=MESH)

    forward_dev = (after, h)
    backward_dev = (before, (CHIPS - 1) * 2 + h)

    @pl.when(y == CHIPS - 1)
    def _():
        halo_x(forward_dev, me).start()
        halo_b(forward_dev, me).start()

    @pl.when(y == 0)
    def _():
        halo_x(backward_dev, me).start()
        halo_b(backward_dev, me).start()

    def flag_copy(k):
        return pltpu.make_async_remote_copy(
            flag_ref.at[me], flag_ref.at[me], flag_send.at[k], flag_recv.at[k],
            device_id=(g, (me + k) % 8), device_id_type=MESH)

    def flag_arrival(k):
        src = (me + 8 - k) % 8
        return pltpu.make_async_remote_copy(
            flag_ref.at[src], flag_ref.at[src], flag_send.at[k], flag_recv.at[k],
            device_id=(g, src), device_id_type=MESH)

    for k in range(1, 8):
        flag_copy(k).start()

    sig = sig_ref[0]
    passes = functools.partial(
        tile_pass, l_ref=l_ref, r_ref=r_ref, k_ref=k_ref, v_ref=v_ref, p_ref=p_ref, s_ref=s_ref,
        sig=sig, sq_ref=sq_ref, h_ref=h_ref)

    passes(0, ch, bs)

    for k in range(1, 8):
        flag_arrival(k).wait_recv()
    total_flags = flag_ref[0]
    for k in range(1, 8):
        total_flags = total_flags + flag_ref[k]
    group_ref[0] = total_flags
    group_copy = pltpu.make_async_remote_copy(
        group_ref.at[0], group_ref.at[1], flag_send.at[0], flag_recv.at[0],
        device_id=forward_dev, device_id_type=MESH)

    @pl.when(y == CHIPS - 1)
    def _():
        group_copy.start()

    load_x1.wait()
    prepare(1)
    v_ref[:, bs : 2 * bs] = b_ref[:, block(first)].astype(jnp.bfloat16)
    passes(1, ch, bs)

    @pl.when(jnp.logical_not(edge))
    def _():
        load_x2.wait()
        load_bh.wait()

    @pl.when(edge)
    def _():
        pass_on(x_ref, half_x, 0, h).wait_recv()
        pass_on(x_ref, half_x, 0, h).start()
        pass_on(bh_ref, half, 1, h).wait_recv()
        pass_on(bh_ref, half, 1, h).start()
        pass_on(x_ref, other_x, 0, 1 - h).wait_recv()
        pass_on(bh_ref, other, 1, 1 - h).wait_recv()

    prepare(2)
    v_ref[:, 2 * bs : 3 * bs] = bh_ref[...].astype(jnp.bfloat16)
    passes(2, ch, bs)

    @pl.when(y == 0)
    def _():
        group_copy.wait_recv()

    load_noise.wait()
    flag_first = group_ref[0, pl.ds(jnp.maximum(y - 1, 0), 1), :]

    @pl.when(y > 0)
    def _():
        group_ref[2, 0:1, :] = group_ref[0, pl.ds(y, 1), :]

    @pl.when(y == 0)
    def _():
        group_ref[2, 0:1, :] = group_ref[1, CHIPS - 1 : CHIPS, :]

    flag_last = group_ref[2, 0:1, :]
    flag_first = jnp.tile(flag_first, (1, own // 128))
    flag_last = jnp.tile(flag_last, (1, own // 128))
    diagonal = noise_ref[...] + flag_first * s_ref[1, 0:1, :] + flag_last * s_ref[2, 0:1, :]

    def image(vec):
        return diagonal * vec + (p_ref[0] + flag_first * p_ref[1] + flag_last * p_ref[2])

    lane = lax.broadcasted_iota(jnp.int32, (R, 128), 1)

    def set_stats(t, arrays):
        stats = jnp.zeros((R, 128), jnp.float32)
        for k, a in enumerate(arrays):
            stats = jnp.where(lane == k, jnp.sum(a, axis=1, keepdims=True), stats)
        padded = jnp.concatenate([stats, jnp.zeros((128 - R, 128), jnp.float32)], 0)
        st_ref[t, me] = padded.T[0:8]

    def sum_copies(t, ref, stage, n, place, device_of):
        def send(k):
            return pltpu.make_async_remote_copy(
                ref.at[t, place], ref.at[t, place], sum_send.at[t, stage, k], sum_recv.at[t, stage, k],
                device_id=device_of((place + k) % n), device_id_type=MESH)

        def arrival(k):
            src = (place + n - k) % n
            return pltpu.make_async_remote_copy(
                ref.at[t, src], ref.at[t, src], sum_send.at[t, stage, k], sum_recv.at[t, stage, k],
                device_id=device_of(src), device_id_type=MESH)

        def start():
            for k in range(1, n):
                send(k).start()

        def finish():
            for k in range(1, n):
                arrival(k).wait_recv()
            total = ref[t, 0]
            for k in range(1, n):
                total = total + ref[t, k]
            return total

        def drain():
            for k in range(1, n):
                send(k).wait_send()

        return start, finish, drain

    def stages(t):
        return (
            sum_copies(t, st_ref, 0, 8, me, lambda p: (g, p)),
            sum_copies(t, sx_ref, 1, nx, gx, lambda p: (p * nz + gz, me)),
            sum_copies(t, sz_ref, 2, nz, gz, lambda p: (gx * nz + p, me)),
        )

    def part_copy(t, ref, which, k, device):
        return pltpu.make_async_remote_copy(
            ref.at[:, piece(which)], ref.at[:, piece(which)], part_send.at[t, k], part_recv.at[t, which],
            device_id=device, device_id_type=MESH)

    def parts(t, ref):
        to_up, to_down = (g, up * 2 + h), (g, down * 2 + h)
        sends = [
            part_copy(t, ref, me, 0, to_up),
            part_copy(t, ref, me, 1, to_down),
            part_copy(t, ref, me, 2, partner),
            part_copy(t, ref, down * 2 + h, 3, partner),
            part_copy(t, ref, up * 2 + h, 4, partner),
            part_copy(t, ref, across * 2 + h, 5, partner),
        ]
        relay_up = part_copy(t, ref, down * 2 + h, 6, to_up)
        relay_down = part_copy(t, ref, up * 2 + h, 6, to_down)

        def arrived(which):
            part_copy(t, ref, which, 0, partner).wait_recv()

        def begin():
            for s in sends[:3]:
                s.start()

        def relay():
            arrived(down * 2 + h)

            @pl.when(h == 0)
            def _():
                relay_up.start()

            sends[3].start()
            arrived(up * 2 + h)

            @pl.when(h == 1)
            def _():
                relay_down.start()

            sends[4].start()

        def near():
            arrived(y * 2 + 1 - h)
            arrived(down * 2 + 1 - h)
            arrived(up * 2 + 1 - h)

        def far():
            arrived(across * 2 + h)
            sends[5].start()
            arrived(across * 2 + 1 - h)

        def drain():
            for s in sends:
                s.wait_send()
            relay_up.wait_send()

        return begin, relay, near, far, drain

    b_own = b_ref[:, mine]
    q_own = image(b_own)
    q1_ref[:, mine] = q_own
    set_stats(0, (b_own * b_own, b_own * q_own, q_own * q_own))

    (a_start, a_finish, a_drain), (x_start, x_finish, x_drain), (z_start, z_finish, z_drain) = stages(0)
    begin, relay, near, far, drain = parts(0, q1_ref)
    a_start()
    begin()

    @pl.when(y == CHIPS - 1)
    def _():
        halo_q(forward_dev).start()

    @pl.when(y == 0)
    def _():
        halo_q(backward_dev).start()

    sx_ref[0, gx] = a_finish()
    x_start()
    sz_ref[0, gz] = x_finish()
    z_start()
    relay()

    @pl.when(edge)
    def _():
        pass_on(qh_ref, half, 2, h).wait_recv()
        pass_on(qh_ref, half, 2, h).start()

    total = z_finish()
    norm, curve, square = total[0:1], total[1:2], total[2:3]
    step1 = norm / curve
    norm2 = norm - 2.0 * step1 * curve + step1 * step1 * square
    ratio = norm2 / norm

    def as_columns(rows):
        stacked = jnp.zeros((8, 128), jnp.float32)
        for k, a in enumerate(rows):
            stacked = jnp.where(row == k, a, stacked)
        turned = jnp.concatenate([stacked, jnp.zeros((120, 128), jnp.float32)], 0).T
        return [turned[0:R, k : k + 1] for k in range(len(rows))]

    step1_col, ratio_col = as_columns((step1, ratio))
    near()

    @pl.when(edge)
    def _():
        pass_on(qh_ref, other, 2, 1 - h).wait_recv()

    @pl.when(jnp.logical_not(edge))
    def _():
        qh_ref[...] = q1_ref[:, block(last)]

    def next_direction(b, q):
        return (b - step1_col * q) + ratio_col * b

    v_ref[:, 0:bs] = next_direction(b_ref[:, block(y)], q1_ref[:, block(y)]).astype(jnp.bfloat16)
    v_ref[:, bs : 2 * bs] = next_direction(b_ref[:, block(first)], q1_ref[:, block(first)]).astype(jnp.bfloat16)
    v_ref[:, 2 * bs : 3 * bs] = next_direction(bh_ref[...], qh_ref[...]).astype(jnp.bfloat16)

    def lanes(j, _):
        cols = pl.ds(pl.multiple_of(j * LANES, LANES), LANES)
        for slot in range(3):
            at = pl.ds(slot * bs, bs)
            p_ref[slot, :, cols] = jnp.dot(v_ref[:, at], k_ref[at, cols], preferred_element_type=jnp.float32)
        return 0

    lax.fori_loop(0, own // LANES, lanes, 0)
    d_own = next_direction(b_own, q1_ref[:, mine])
    q2_own = image(d_own)
    q2_ref[:, mine] = q2_own
    set_stats(1, (d_own * q2_own,))
    (a2_start, a2_finish, a2_drain), (x2_start, x2_finish, x2_drain), (z2_start, z2_finish, z2_drain) = stages(1)
    begin2, relay2, near2, far2, drain2 = parts(1, q2_ref)
    a2_start()
    begin2()
    far()
    sx_ref[1, gx] = a2_finish()
    x2_start()
    sz_ref[1, gz] = x2_finish()
    z2_start()
    relay2()
    far2()
    total2 = z2_finish()
    (step2_col,) = as_columns((norm2 / total2[0:1],))
    near2()

    outs = []
    for i in range(CHIPS):
        at = pl.ds(i * bs, bs)
        b = b_ref[:, at]
        r1 = b - step1_col * q1_ref[:, at]
        d2 = r1 + ratio_col * b
        sol_ref[:, at] = step1_col * b + step2_col * d2
        res_ref[:, at] = r1 - step2_col * q2_ref[:, at]
        outs.append(pltpu.make_async_copy(sol_ref.at[:, at], sol_hbm.at[:, at], out_sem.at[2 * i]))
        outs.append(pltpu.make_async_copy(res_ref.at[:, at], res_hbm.at[:, at], out_sem.at[2 * i + 1]))
        outs[-2].start()
        outs[-1].start()

    for k in range(1, 8):
        flag_copy(k).wait_send()
    for wait in (a_drain, x_drain, z_drain, drain, a2_drain, x2_drain, z2_drain, drain2):
        wait()

    @pl.when(edge)
    def _():
        halo_x(forward_dev, me).wait_send()
        halo_b(forward_dev, me).wait_send()
        halo_q(forward_dev).wait_send()
        pass_on(x_ref, half_x, 0, h).wait_send()
        pass_on(bh_ref, half, 1, h).wait_send()
        pass_on(qh_ref, half, 2, h).wait_send()

    @pl.when(y == CHIPS - 1)
    def _():
        group_copy.wait_send()

    for o in outs:
        o.wait()


def body(features, inv_scale, signal, noise_var, right_side, block_pairs):
    local = features.shape[1]
    bs = local // CHIPS
    own = bs // 2
    nx, nz = TORUS[lax.axis_size("blk")]
    inv = jnp.broadcast_to((inv_scale * (W / 16.0))[:, None], (F, 128))
    vmem = pltpu.VMEM
    dma = pltpu.SemaphoreType.DMA
    f32, bf16 = jnp.float32, jnp.bfloat16
    hbm = pl.BlockSpec(memory_space=pl.ANY)
    smem = pl.BlockSpec(memory_space=pltpu.SMEM)
    shape = jax.ShapeDtypeStruct(right_side.shape, f32)
    return pl.pallas_call(
        functools.partial(kernel, nx, nz, bs),
        name="conjugate_gradients",
        out_shape=(shape, shape),
        in_specs=[hbm, pl.BlockSpec(memory_space=pltpu.VMEM), smem, hbm, hbm, smem],
        out_specs=(hbm, hbm),
        scratch_shapes=[
            vmem((F, 3 * bs), f32),
            vmem((3 * bs, TERMS), bf16),
            vmem((TERMS, own), bf16),
            vmem((3 * bs, own), bf16),
            vmem((R, local), f32),
            vmem((R, bs), f32),
            vmem((R, local), f32),
            vmem((R, bs), f32),
            vmem((R, local), f32),
            vmem((R, 3 * bs), bf16),
            vmem((3, R, own), f32),
            vmem((3, 8, own), f32),
            vmem((1, own), f32),
            vmem((2, bs // 4, LANES), f32),
            vmem((2, bs // 4, LANES), bf16),
            vmem((8, 8, 128), f32),
            vmem((3, 8, 128), f32),
            vmem((2, 8, 8, 128), f32),
            vmem((2, nx, 8, 128), f32),
            vmem((2, nz, 8, 128), f32),
            vmem((R, local), f32),
            vmem((R, local), f32),
            dma((6,)),
            dma((8,)),
            dma((6,)),
            dma((6,)),
            dma((8,)),
            dma((8,)),
            dma((2, 3, 8)),
            dma((2, 3, 8)),
            dma((2, 7)),
            dma((2, 8)),
        ],
        compiler_params=pltpu.CompilerParams(
            collective_id=0, has_side_effects=True, vmem_limit_bytes=60 * 1024 * 1024
        ),
    )(features, inv, signal, noise_var.reshape(1, -1), right_side, block_pairs)


def solution(mesh):
    placed = (P(None, "blk"), P(), P(), P("blk"), P(None, "blk"), P(("blk", "pair"), None))
    return jax.shard_map(
        body,
        mesh=mesh,
        in_specs=placed,
        out_specs=(P(None, "blk"), P(None, "blk")),
        check_vma=False,
    )
```

```python
import functools
import math

import jax
import jax.numpy as jnp
from jax import lax
from jax.experimental import pallas as pl
from jax.experimental.pallas import tpu as pltpu
from jax.sharding import PartitionSpec as P

F = 64
R = 32
CHIPS = 4
TORUS = {32: (4, 8), 8: (2, 4), 2: (1, 2)}
LANES = 256
TERMS = 512
MESH = pl.DeviceIdType.MESH

ROOT3 = math.sqrt(3.0)
W = 2.0 * ROOT3 * math.log2(math.e)
SCALE = 2.0**-W / W**4
Q0 = 5.0 * (1.0 + 2.0 * ROOT3) * SCALE
Q1 = -(4.0 * (1.0 + 2.0 * ROOT3) + 10.0 * ROOT3) / W * SCALE
Q2 = 8.0 * ROOT3 / W**2 * SCALE
TINY = 1e-30


def split3(s):
    hi = s.astype(jnp.bfloat16)
    rest = s - hi.astype(jnp.float32)
    mid = rest.astype(jnp.bfloat16)
    lo = (rest - mid.astype(jnp.float32)).astype(jnp.bfloat16)
    return hi, mid, lo


def norm_rows(norms, first):
    n = norms.shape[1]
    hi, mid, lo = split3(norms)
    row = lax.broadcasted_iota(jnp.int32, (8, n), 0)
    base = 0 if first else 3
    ones = (row >= 3 - base) & (row < 6 - base)
    top = jnp.where(row == base, hi.astype(jnp.float32), 0.0)
    top = jnp.where(row == base + 1, mid.astype(jnp.float32), top)
    top = jnp.where(row == base + 2, lo.astype(jnp.float32), top)
    top = jnp.where(ones, 1.0, top)
    return jnp.concatenate([top, jnp.zeros((F - 8, n), jnp.float32)], 0).astype(jnp.bfloat16)


def left_terms(x, inv):
    s = x * inv
    norms = jnp.sum(s * s, axis=0, keepdims=True)
    hi, mid, lo = split3(-2.0 * s)
    return jnp.concatenate([hi, mid], 0).T, jnp.concatenate([lo, norm_rows(norms, False)], 0).T


def right_terms(x, inv):
    s = x * inv
    norms = jnp.sum(s * s, axis=0, keepdims=True)
    hi, mid, lo = split3(s)
    return jnp.concatenate([hi, hi, mid, mid, lo, jnp.zeros_like(lo), hi, norm_rows(norms, True)], 0)


def tile_values(sq, c0, c1, c2):
    y = jnp.maximum(sq, TINY)
    w = y * lax.rsqrt(y)
    u = jnp.maximum(W - w, 0.0)
    u2 = u * u
    return ((c2 * u + c1) * u + c0) * jnp.exp2(u) * (u2 * u2)


def tile_pass(slot, ch, bs, l_ref, r_ref, k_ref, v_ref, p_ref, s_ref, sig, sq_ref, h_ref, after=None):
    c0, c1, c2 = sig * Q0, sig * Q1, sig * Q2
    n = bs // ch
    base = slot * bs

    def lanes(j, _):
        cols = pl.ds(pl.multiple_of(j * LANES, LANES), LANES)

        def at(i):
            return pl.ds(pl.multiple_of(base + i * ch, ch), ch)

        def cross(i, buf):
            sq_ref[buf] = jnp.dot(l_ref[at(i), :], r_ref[:, cols], preferred_element_type=jnp.float32)

        def values(i, buf, sums):
            t = tile_values(sq_ref[buf], c0, c1, c2)
            half = t.astype(jnp.bfloat16)
            h_ref[buf] = half
            k_ref[at(i), cols] = half
            return sums + jnp.sum(t.reshape(ch // 8, 8, LANES), axis=0)

        def prod(i, buf, acc):
            return acc + jnp.dot(v_ref[:, at(i)], h_ref[buf], preferred_element_type=jnp.float32)

        acc = jnp.zeros((R, LANES), jnp.float32)
        sums = jnp.zeros((8, LANES), jnp.float32)
        cross(0, 0)
        cross(1, 1)
        sums = values(0, 0, sums)

        def rows(m, carry):
            acc, sums = carry
            i = 2 * m + 1
            cross(i + 1, 0)
            sums = values(i, 1, sums)
            acc = prod(i - 1, 0, acc)
            cross(i + 2, 1)
            sums = values(i + 1, 0, sums)
            acc = prod(i, 1, acc)
            return acc, sums

        acc, sums = lax.fori_loop(0, (n - 2) // 2, rows, (acc, sums))
        sums = values(n - 1, 1, sums)
        acc = prod(n - 2, 0, acc)
        acc = prod(n - 1, 1, acc)
        p_ref[slot, :, cols] = acc
        s_ref[slot, :, cols] = jnp.broadcast_to(jnp.sum(sums, axis=0, keepdims=True), (8, LANES))
        if after is not None:
            after(j, cols)
        return 0

    lax.fori_loop(0, p_ref.shape[2] // LANES, lanes, 0)


def kernel(
    nx, nz, bs,
    x_hbm, inv_ref, sig_ref, noise_hbm, b_hbm, pairs_ref,
    q1_hbm, q2_hbm, coef_ref,
    x_ref, l_ref, r_ref, k_ref, b_ref, bh_ref, q1_ref, qh_ref, q2_ref, v_ref,
    p_ref, s_ref, noise_ref, sq_ref, h_ref, flag_ref, group_ref, st_ref, sx_ref, sz_ref,
    diag_ref,
    local_sem, out_sem, halo_send, halo_recv, edge_send, edge_recv, flag_send, flag_recv, sum_send, sum_recv, part_send, part_recv,
):
    own = bs // 2
    ch = bs // 4
    count = nx * nz
    g = lax.axis_index("blk")
    me = lax.axis_index("pair")
    y, h = me // 2, me % 2
    gx, gz = g // nz, g % nz
    up, down, across = (y + 1) % CHIPS, (y + CHIPS - 1) % CHIPS, (y + 2) % CHIPS
    partner = (g, y * 2 + 1 - h)
    after, before = (g + 1) % count, (g + count - 1) % count
    edge = (y == 0) | (y == CHIPS - 1)
    first = jnp.where(y == 0, 1, y - 1)
    last = jnp.minimum(y + 1, CHIPS - 1)

    def block(i):
        return pl.ds(pl.multiple_of(i * bs, bs), bs)

    def piece(i):
        return pl.ds(pl.multiple_of(i * own, own), own)

    mine = piece(me)

    barrier = pltpu.get_barrier_semaphore()

    def greet(device):
        pl.semaphore_signal(barrier, inc=1, device_id=device, device_id_type=MESH)

    for k in range(1, 8):
        greet((g, (me + k) % 8))
    for k in range(1, nx):
        greet((((gx + k) % nx) * nz + gz, me))
    for k in range(1, nz):
        greet((gx * nz + (gz + k) % nz, me))

    @pl.when(y == CHIPS - 1)
    def _():
        greet((after, h))

    @pl.when(y == 0)
    def _():
        greet((before, (CHIPS - 1) * 2 + h))

    load_x0 = pltpu.make_async_copy(x_hbm.at[:, block(y)], x_ref.at[:, pl.ds(0, bs)], local_sem.at[0])
    load_x1 = pltpu.make_async_copy(x_hbm.at[:, block(first)], x_ref.at[:, pl.ds(bs, bs)], local_sem.at[1])
    load_x2 = pltpu.make_async_copy(x_hbm.at[:, block(last)], x_ref.at[:, pl.ds(2 * bs, bs)], local_sem.at[2])
    load_b = pltpu.make_async_copy(b_hbm, b_ref, local_sem.at[3])
    load_bh = pltpu.make_async_copy(b_hbm.at[:, block(last)], bh_ref, local_sem.at[4])
    load_noise = pltpu.make_async_copy(noise_hbm.at[:, mine], noise_ref, local_sem.at[5])
    load_x0.start()
    load_b.start()
    load_x1.start()
    load_noise.start()

    @pl.when(jnp.logical_not(edge))
    def _():
        load_x2.start()
        load_bh.start()

    row = lax.broadcasted_iota(jnp.int32, (8, 128), 0)
    flags = jnp.zeros((8, 128), jnp.float32)
    for k in range(CHIPS):
        left = g * CHIPS + k
        listed = jnp.float32(0.0)
        for s in range(2):
            hit = (pairs_ref[s, 0] == left) & (pairs_ref[s, 1] == left + 1)
            listed = listed + jnp.where(hit, 1.0, 0.0)
        flags = jnp.where(row == k, listed, flags)
    flag_ref[me] = flags

    scale = inv_ref[...] * (W / 16.0)
    scale = jnp.broadcast_to(jnp.concatenate([scale, scale], 1), (128, 2 * F)).T[0:F]
    inv = jnp.tile(scale, (1, ch // 128))

    def prepare(slot):
        def part(i, _):
            at = pl.ds(pl.multiple_of(slot * bs + i * ch, ch), ch)
            a, c = left_terms(x_ref[:, at], inv)
            l_ref[at, 0:128] = a
            l_ref[at, 128:256] = a
            l_ref[at, 256:384] = a
            l_ref[at, 384:512] = c
            return 0

        lax.fori_loop(0, bs // ch, part, 0)

    load_x0.wait()
    prepare(0)
    for i in range(own // ch):
        at = pl.ds(pl.multiple_of(h * own + i * ch, ch), ch)
        r_ref[:, i * ch : (i + 1) * ch] = right_terms(x_ref[:, at], inv)
    load_b.wait()
    v_ref[:, 0:bs] = b_ref[:, block(y)].astype(jnp.bfloat16)
    v_ref[:, bs : 2 * bs] = b_ref[:, block(first)].astype(jnp.bfloat16)
    load_x1.wait()
    prepare(1)

    pl.semaphore_wait(barrier, 5 + nx + nz + jnp.where(edge, 1, 0))

    half = pl.ds(pl.multiple_of(h * own, own), own)
    half_x = pl.ds(pl.multiple_of(2 * bs + h * own, own), own)
    other = pl.ds(pl.multiple_of((1 - h) * own, own), own)
    other_x = pl.ds(pl.multiple_of(2 * bs + (1 - h) * own, own), own)

    def halo_x(device, src):
        return pltpu.make_async_remote_copy(
            x_hbm.at[:, piece(src)], x_ref.at[:, half_x], halo_send.at[0], halo_recv.at[h],
            device_id=device, device_id_type=MESH)

    def halo_b(device, src):
        return pltpu.make_async_remote_copy(
            b_hbm.at[:, piece(src)], bh_ref.at[:, half], halo_send.at[1], halo_recv.at[2 + h],
            device_id=device, device_id_type=MESH)

    chunks = own // LANES

    def slab(i, c):
        return pl.ds(pl.multiple_of(i * own + c * LANES, LANES), LANES)

    def edge_q(device, c):
        return pltpu.make_async_remote_copy(
            q1_ref.at[:, slab(me, c)], qh_ref.at[:, slab(h, c)], edge_send.at[0, c], edge_recv.at[h, c],
            device_id=device, device_id_type=MESH)

    def edge_on(side, c):
        return pltpu.make_async_remote_copy(
            qh_ref.at[:, slab(side, c)], qh_ref.at[:, slab(side, c)], edge_send.at[1, c], edge_recv.at[side, c],
            device_id=partner, device_id_type=MESH)

    def pass_on(ref, at, k, sem):
        return pltpu.make_async_remote_copy(
            ref.at[:, at], ref.at[:, at], halo_send.at[2 + k], halo_recv.at[2 * k + sem],
            device_id=partner, device_id_type=MESH)

    forward_dev = (after, h)
    backward_dev = (before, (CHIPS - 1) * 2 + h)

    @pl.when(y == CHIPS - 1)
    def _():
        halo_x(forward_dev, me).start()
        halo_b(forward_dev, me).start()

    @pl.when(y == 0)
    def _():
        halo_x(backward_dev, me).start()
        halo_b(backward_dev, me).start()

    def flag_copy(k):
        return pltpu.make_async_remote_copy(
            flag_ref.at[me], flag_ref.at[me], flag_send.at[k], flag_recv.at[k],
            device_id=(g, (me + k) % 8), device_id_type=MESH)

    def flag_arrival(k):
        src = (me + 8 - k) % 8
        return pltpu.make_async_remote_copy(
            flag_ref.at[src], flag_ref.at[src], flag_send.at[k], flag_recv.at[k],
            device_id=(g, src), device_id_type=MESH)

    for k in range(1, 8):
        flag_copy(k).start()

    sig = sig_ref[0]
    passes = functools.partial(
        tile_pass, l_ref=l_ref, r_ref=r_ref, k_ref=k_ref, v_ref=v_ref, p_ref=p_ref, s_ref=s_ref,
        sig=sig, sq_ref=sq_ref, h_ref=h_ref)

    passes(0, ch, bs)

    for k in range(1, 8):
        flag_arrival(k).wait_recv()
    total_flags = flag_ref[0]
    for k in range(1, 8):
        total_flags = total_flags + flag_ref[k]
    group_ref[0] = total_flags
    group_copy = pltpu.make_async_remote_copy(
        group_ref.at[0], group_ref.at[1], flag_send.at[0], flag_recv.at[0],
        device_id=forward_dev, device_id_type=MESH)

    @pl.when(y == CHIPS - 1)
    def _():
        group_copy.start()

    passes(1, ch, bs)

    @pl.when(jnp.logical_not(edge))
    def _():
        load_x2.wait()
        load_bh.wait()

    @pl.when(edge)
    def _():
        pass_on(x_ref, half_x, 0, h).wait_recv()
        pass_on(x_ref, half_x, 0, h).start()
        pass_on(bh_ref, half, 1, h).wait_recv()
        pass_on(bh_ref, half, 1, h).start()
        pass_on(x_ref, other_x, 0, 1 - h).wait_recv()
        pass_on(bh_ref, other, 1, 1 - h).wait_recv()

    prepare(2)
    v_ref[:, 2 * bs : 3 * bs] = bh_ref[...].astype(jnp.bfloat16)
    load_noise.wait()

    @pl.when(y == 0)
    def _():
        group_copy.wait_recv()
        group_ref[2, 0:1, :] = group_ref[1, CHIPS - 1 : CHIPS, :]

    @pl.when(y > 0)
    def _():
        group_ref[2, 0:1, :] = group_ref[0, pl.ds(y, 1), :]

    flag_first = jnp.tile(group_ref[0, pl.ds(jnp.maximum(y - 1, 0), 1), :], (1, LANES // 128))
    flag_last = jnp.tile(group_ref[2, 0:1, :], (1, LANES // 128))

    to_up, to_down = (g, up * 2 + h), (g, down * 2 + h)

    def part_copy(t, ref, which, c, k, device):
        return pltpu.make_async_remote_copy(
            ref.at[:, slab(which, c)], ref.at[:, slab(which, c)], part_send.at[t, k, c], part_recv.at[t, which, c],
            device_id=device, device_id_type=MESH)

    def hand_out(t, ref, c):
        part_copy(t, ref, me, c, 0, to_up).start()
        part_copy(t, ref, me, c, 1, to_down).start()
        part_copy(t, ref, me, c, 2, partner).start()

    def image(cols, vec):
        return diag_ref[:, cols] * vec + (p_ref[0, :, cols] + flag_first * p_ref[1, :, cols] + flag_last * p_ref[2, :, cols])

    def first_image(j, cols):
        at = slab(me, j)
        diag_ref[:, cols] = noise_ref[:, cols] + flag_first * s_ref[1, 0:1, cols] + flag_last * s_ref[2, 0:1, cols]
        q1_ref[:, at] = image(cols, b_ref[:, at])
        hand_out(0, q1_ref, j)

        @pl.when(y == CHIPS - 1)
        def _():
            edge_q(forward_dev, j).start()

        @pl.when(y == 0)
        def _():
            edge_q(backward_dev, j).start()

    passes(2, ch, bs, after=first_image)

    lane = lax.broadcasted_iota(jnp.int32, (R, 128), 1)

    def set_stats(t, arrays):
        stats = jnp.zeros((R, 128), jnp.float32)
        for k, a in enumerate(arrays):
            stats = jnp.where(lane == k, jnp.sum(a, axis=1, keepdims=True), stats)
        padded = jnp.concatenate([stats, jnp.zeros((128 - R, 128), jnp.float32)], 0)
        st_ref[t, me] = padded.T[0:8]

    def sum_copies(t, ref, stage, n, place, device_of):
        def send(k):
            return pltpu.make_async_remote_copy(
                ref.at[t, place], ref.at[t, place], sum_send.at[t, stage, k], sum_recv.at[t, stage, k],
                device_id=device_of((place + k) % n), device_id_type=MESH)

        def arrival(k):
            src = (place + n - k) % n
            return pltpu.make_async_remote_copy(
                ref.at[t, src], ref.at[t, src], sum_send.at[t, stage, k], sum_recv.at[t, stage, k],
                device_id=device_of(src), device_id_type=MESH)

        def start():
            for k in range(1, n):
                send(k).start()

        def finish():
            for k in range(1, n):
                arrival(k).wait_recv()
            total = ref[t, 0]
            for k in range(1, n):
                total = total + ref[t, k]
            return total

        def drain():
            for k in range(1, n):
                send(k).wait_send()

        return start, finish, drain

    def stages(t):
        return (
            sum_copies(t, st_ref, 0, 8, me, lambda p: (g, p)),
            sum_copies(t, sx_ref, 1, nx, gx, lambda p: (p * nz + gz, me)),
            sum_copies(t, sz_ref, 2, nz, gz, lambda p: (gx * nz + p, me)),
        )

    def parts(t, ref):
        def arrived(which, c):
            part_copy(t, ref, which, c, 0, partner).wait_recv()

        def relay():
            for c in range(chunks):
                arrived(down * 2 + h, c)

                @pl.when(h == 0)
                def _():
                    part_copy(t, ref, down * 2 + h, c, 6, to_up).start()

                part_copy(t, ref, down * 2 + h, c, 3, partner).start()
                arrived(up * 2 + h, c)

                @pl.when(h == 1)
                def _():
                    part_copy(t, ref, up * 2 + h, c, 6, to_down).start()

                part_copy(t, ref, up * 2 + h, c, 4, partner).start()

        def near():
            for c in range(chunks):
                arrived(y * 2 + 1 - h, c)
                arrived(down * 2 + 1 - h, c)
                arrived(up * 2 + 1 - h, c)

        def far_on():
            for c in range(chunks):
                arrived(across * 2 + h, c)
                part_copy(t, ref, across * 2 + h, c, 5, partner).start()

        def far():
            for c in range(chunks):
                arrived(across * 2 + 1 - h, c)

        def drain():
            for c in range(chunks):
                for k in range(7):
                    part_copy(t, ref, me, c, k, partner).wait_send()

        return relay, near, far_on, far, drain

    b_own = b_ref[:, mine]
    q_own = q1_ref[:, mine]
    set_stats(0, (b_own * b_own, b_own * q_own, q_own * q_own))
    (a_start, a_finish, a_drain), (x_start, x_finish, x_drain), (z_start, z_finish, z_drain) = stages(0)
    relay, near, far_on, far, drain = parts(0, q1_ref)
    a_start()
    sx_ref[0, gx] = a_finish()
    x_start()
    relay()

    @pl.when(edge)
    def _():
        for c in range(chunks):
            edge_on(h, c).wait_recv()
            edge_on(h, c).start()

    sz_ref[0, gz] = x_finish()
    z_start()
    far_on()

    total = z_finish()
    norm, curve, square = total[0:1], total[1:2], total[2:3]
    step1 = norm / curve
    norm2 = norm - 2.0 * step1 * curve + step1 * step1 * square
    ratio = norm2 / norm

    def as_columns(rows):
        stacked = jnp.zeros((8, 128), jnp.float32)
        for k, a in enumerate(rows):
            stacked = jnp.where(row == k, a, stacked)
        turned = jnp.concatenate([stacked, jnp.zeros((120, 128), jnp.float32)], 0).T
        return [turned[0:R, k : k + 1] for k in range(len(rows))]

    step1_col, ratio_col = as_columns((step1, ratio))
    near()

    @pl.when(edge)
    def _():
        for c in range(chunks):
            edge_on(1 - h, c).wait_recv()

    @pl.when(jnp.logical_not(edge))
    def _():
        qh_ref[...] = q1_ref[:, block(last)]

    def next_direction(b, q):
        return (b - step1_col * q) + ratio_col * b

    v_ref[:, 0:bs] = next_direction(b_ref[:, block(y)], q1_ref[:, block(y)]).astype(jnp.bfloat16)
    v_ref[:, bs : 2 * bs] = next_direction(b_ref[:, block(first)], q1_ref[:, block(first)]).astype(jnp.bfloat16)
    v_ref[:, 2 * bs : 3 * bs] = next_direction(bh_ref[...], qh_ref[...]).astype(jnp.bfloat16)

    def lanes(j, _):
        cols = pl.ds(pl.multiple_of(j * LANES, LANES), LANES)
        for slot in range(3):
            rows = pl.ds(slot * bs, bs)
            p_ref[slot, :, cols] = jnp.dot(v_ref[:, rows], k_ref[rows, cols], preferred_element_type=jnp.float32)
        at = slab(me, j)
        q2_ref[:, at] = image(cols, next_direction(b_ref[:, at], q1_ref[:, at]))
        hand_out(1, q2_ref, j)
        return 0

    lax.fori_loop(0, chunks, lanes, 0)
    d_own = next_direction(b_own, q1_ref[:, mine])
    set_stats(1, (d_own * q2_ref[:, mine],))
    (a2_start, a2_finish, a2_drain), (x2_start, x2_finish, x2_drain), (z2_start, z2_finish, z2_drain) = stages(1)
    relay2, near2, far_on2, far2, drain2 = parts(1, q2_ref)
    a2_start()
    far()
    q1_out = pltpu.make_async_copy(q1_ref, q1_hbm, out_sem.at[0])
    q1_out.start()
    sx_ref[1, gx] = a2_finish()
    x2_start()
    relay2()
    sz_ref[1, gz] = x2_finish()
    z2_start()
    far_on2()
    near2()
    far2()
    q2_out = pltpu.make_async_copy(q2_ref, q2_hbm, out_sem.at[1])
    q2_out.start()
    total2 = z2_finish()
    (step2_col,) = as_columns((norm2 / total2[0:1],))
    coef_ref[...] = jnp.where(lane == 0, step1_col, jnp.where(lane == 1, ratio_col, step2_col))

    for k in range(1, 8):
        flag_copy(k).wait_send()
    for wait in (a_drain, x_drain, z_drain, drain, a2_drain, x2_drain, z2_drain, drain2):
        wait()

    @pl.when(edge)
    def _():
        halo_x(forward_dev, me).wait_send()
        halo_b(forward_dev, me).wait_send()
        pass_on(x_ref, half_x, 0, h).wait_send()
        pass_on(bh_ref, half, 1, h).wait_send()
        for c in range(chunks):
            edge_q(forward_dev, c).wait_send()
            edge_on(h, c).wait_send()

    @pl.when(y == CHIPS - 1)
    def _():
        group_copy.wait_send()

    q1_out.wait()
    q2_out.wait()


def body(features, inv_scale, signal, noise_var, right_side, block_pairs):
    local = features.shape[1]
    bs = local // CHIPS
    own = bs // 2
    nx, nz = TORUS[lax.axis_size("blk")]
    vmem = pltpu.VMEM
    dma = pltpu.SemaphoreType.DMA
    f32, bf16 = jnp.float32, jnp.bfloat16
    hbm = pl.BlockSpec(memory_space=pl.ANY)
    smem = pl.BlockSpec(memory_space=pltpu.SMEM)
    shape = jax.ShapeDtypeStruct(right_side.shape, f32)
    q1, q2, coef = pl.pallas_call(
        functools.partial(kernel, nx, nz, bs),
        name="conjugate_gradients",
        out_shape=(shape, shape, jax.ShapeDtypeStruct((R, 128), f32)),
        in_specs=[hbm, pl.BlockSpec(memory_space=pltpu.VMEM), smem, hbm, hbm, smem],
        out_specs=(hbm, hbm, pl.BlockSpec(memory_space=pltpu.VMEM)),
        scratch_shapes=[
            vmem((F, 3 * bs), f32),
            vmem((3 * bs, TERMS), bf16),
            vmem((TERMS, own), bf16),
            vmem((3 * bs, own), bf16),
            vmem((R, local), f32),
            vmem((R, bs), f32),
            vmem((R, local), f32),
            vmem((R, bs), f32),
            vmem((R, local), f32),
            vmem((R, 3 * bs), bf16),
            vmem((3, R, own), f32),
            vmem((3, 8, own), f32),
            vmem((1, own), f32),
            vmem((2, bs // 4, LANES), f32),
            vmem((2, bs // 4, LANES), bf16),
            vmem((8, 8, 128), f32),
            vmem((3, 8, 128), f32),
            vmem((2, 8, 8, 128), f32),
            vmem((2, nx, 8, 128), f32),
            vmem((2, nz, 8, 128), f32),
            vmem((1, own), f32),
            dma((6,)),
            dma((2,)),
            dma((4,)),
            dma((4,)),
            dma((2, own // LANES)),
            dma((2, own // LANES)),
            dma((8,)),
            dma((8,)),
            dma((2, 3, 8)),
            dma((2, 3, 8)),
            dma((2, 7, own // LANES)),
            dma((2, 8, own // LANES)),
        ],
        compiler_params=pltpu.CompilerParams(
            collective_id=0, has_side_effects=True, vmem_limit_bytes=60 * 1024 * 1024
        ),
    )(features, inv_scale.reshape(1, -1), signal, noise_var.reshape(1, -1), right_side, block_pairs)
    step1, ratio, step2 = coef[:, 0:1], coef[:, 1:2], coef[:, 2:3]
    residual = right_side - step1 * q1
    return step1 * right_side + step2 * (residual + ratio * right_side), residual - step2 * q2


def solution(mesh):
    placed = (P(None, "blk"), P(), P(), P("blk"), P(None, "blk"), P(("blk", "pair"), None))
    return jax.shard_map(
        body,
        mesh=mesh,
        in_specs=placed,
        out_specs=(P(None, "blk"), P(None, "blk")),
        check_vma=False,
    )
```

```python
import functools
import math

import jax
import jax.numpy as jnp
from jax import lax
from jax.experimental import pallas as pl
from jax.experimental.pallas import tpu as pltpu
from jax.sharding import PartitionSpec as P

F = 64
R = 32
CHIPS = 4
TORUS = {32: (4, 8), 8: (2, 4), 2: (1, 2)}
LANES = 256
TERMS = 512
MESH = pl.DeviceIdType.MESH

ROOT3 = math.sqrt(3.0)
W = 2.0 * ROOT3 * math.log2(math.e)
SCALE = 2.0**-W / W**4
Q0 = 5.0 * (1.0 + 2.0 * ROOT3) * SCALE
Q1 = -(4.0 * (1.0 + 2.0 * ROOT3) + 10.0 * ROOT3) / W * SCALE
Q2 = 8.0 * ROOT3 / W**2 * SCALE
TINY = 1e-30


def split3(s):
    hi = s.astype(jnp.bfloat16)
    rest = s - hi.astype(jnp.float32)
    mid = rest.astype(jnp.bfloat16)
    lo = (rest - mid.astype(jnp.float32)).astype(jnp.bfloat16)
    return hi, mid, lo


def norm_rows(norms, first):
    n = norms.shape[1]
    hi, mid, lo = split3(norms)
    row = lax.broadcasted_iota(jnp.int32, (8, n), 0)
    base = 0 if first else 3
    ones = (row >= 3 - base) & (row < 6 - base)
    top = jnp.where(row == base, hi.astype(jnp.float32), 0.0)
    top = jnp.where(row == base + 1, mid.astype(jnp.float32), top)
    top = jnp.where(row == base + 2, lo.astype(jnp.float32), top)
    top = jnp.where(ones, 1.0, top)
    return jnp.concatenate([top, jnp.zeros((F - 8, n), jnp.float32)], 0).astype(jnp.bfloat16)


def left_terms(x, inv):
    s = x * inv
    norms = jnp.sum(s * s, axis=0, keepdims=True)
    hi, mid, lo = split3(-2.0 * s)
    return jnp.concatenate([hi, mid], 0).T, jnp.concatenate([lo, norm_rows(norms, False)], 0).T


def right_terms(x, inv):
    s = x * inv
    norms = jnp.sum(s * s, axis=0, keepdims=True)
    hi, mid, lo = split3(s)
    return jnp.concatenate([hi, hi, mid, mid, lo, jnp.zeros_like(lo), hi, norm_rows(norms, True)], 0)


def tile_values(sq, c0, c1, c2):
    y = jnp.maximum(sq, TINY)
    w = y * lax.rsqrt(y)
    u = jnp.maximum(W - w, 0.0)
    u2 = u * u
    return ((c2 * u + c1) * u + c0) * jnp.exp2(u) * (u2 * u2)


def tile_pass(slot, ch, bs, l_ref, r_ref, k_ref, v_ref, p_ref, s_ref, sig, sq_ref, h_ref, multiply=True):
    c0, c1, c2 = sig * Q0, sig * Q1, sig * Q2
    n = bs // ch
    base = slot * bs

    def lanes(j, _):
        cols = pl.ds(pl.multiple_of(j * LANES, LANES), LANES)

        def at(i):
            return pl.ds(pl.multiple_of(base + i * ch, ch), ch)

        def cross(i, buf):
            sq_ref[buf] = jnp.dot(l_ref[at(i), :], r_ref[:, cols], preferred_element_type=jnp.float32)

        def values(i, buf, sums):
            t = tile_values(sq_ref[buf], c0, c1, c2)
            half = t.astype(jnp.bfloat16)
            k_ref[at(i), cols] = half
            if multiply:
                h_ref[buf] = half
            if slot == 0:
                return sums
            return sums + jnp.sum(t.reshape(ch // 8, 8, LANES), axis=0)

        def prod(i, buf, acc):
            if not multiply:
                return acc
            return acc + jnp.dot(v_ref[0:R, at(i)], h_ref[buf], preferred_element_type=jnp.float32)

        acc = jnp.zeros((R, LANES), jnp.float32)
        sums = jnp.zeros((8, LANES), jnp.float32)
        cross(0, 0)
        cross(1, 1)
        sums = values(0, 0, sums)

        def rows(m, carry):
            acc, sums = carry
            i = 2 * m + 1
            cross(i + 1, 0)
            sums = values(i, 1, sums)
            acc = prod(i - 1, 0, acc)
            cross(i + 2, 1)
            sums = values(i + 1, 0, sums)
            acc = prod(i, 1, acc)
            return acc, sums

        acc, sums = lax.fori_loop(0, (n - 2) // 2, rows, (acc, sums))
        sums = values(n - 1, 1, sums)
        acc = prod(n - 2, 0, acc)
        acc = prod(n - 1, 1, acc)
        if multiply:
            p_ref[slot, :, cols] = acc
        s_ref[slot, :, cols] = jnp.broadcast_to(jnp.sum(sums, axis=0, keepdims=True), (8, LANES))
        return 0

    lax.fori_loop(0, p_ref.shape[2] // LANES, lanes, 0)


def kernel(
    nx, nz, bs,
    x_hbm, inv_ref, sig_ref, noise_hbm, b_hbm, pairs_ref,
    q1_hbm, q2_hbm, coef_ref,
    x_ref, l_ref, r_ref, k_ref, b_ref, bh_ref, q1_ref, qh_ref, q2_ref, v_ref,
    p_ref, s_ref, noise_ref, sq_ref, h_ref, flag_ref, group_ref, st_ref, sx_ref, sz_ref,
    diag_ref,
    local_sem, out_sem, halo_send, halo_recv, edge_send, edge_recv, flag_send, flag_recv, sum_send, sum_recv, part_send, part_recv,
):
    own = bs // 2
    ch = bs // 4
    count = nx * nz
    g = lax.axis_index("blk")
    me = lax.axis_index("pair")
    y, h = me // 2, me % 2
    gx, gz = g // nz, g % nz
    up, down, across = (y + 1) % CHIPS, (y + CHIPS - 1) % CHIPS, (y + 2) % CHIPS
    partner = (g, y * 2 + 1 - h)
    after, before = (g + 1) % count, (g + count - 1) % count
    edge = (y == 0) | (y == CHIPS - 1)
    first = jnp.where(y == 0, 1, y - 1)
    last = jnp.minimum(y + 1, CHIPS - 1)

    def block(i):
        return pl.ds(pl.multiple_of(i * bs, bs), bs)

    def piece(i):
        return pl.ds(pl.multiple_of(i * own, own), own)

    mine = piece(me)

    barrier = pltpu.get_barrier_semaphore()

    def greet(device):
        pl.semaphore_signal(barrier, inc=1, device_id=device, device_id_type=MESH)

    for k in range(1, 8):
        greet((g, (me + k) % 8))
    for k in range(1, nx):
        greet((((gx + k) % nx) * nz + gz, me))
    for k in range(1, nz):
        greet((gx * nz + (gz + k) % nz, me))

    @pl.when(y == CHIPS - 1)
    def _():
        greet((after, h))

    @pl.when(y == 0)
    def _():
        greet((before, (CHIPS - 1) * 2 + h))

    load_x0 = pltpu.make_async_copy(x_hbm.at[:, block(y)], x_ref.at[:, pl.ds(0, bs)], local_sem.at[0])
    load_x1 = pltpu.make_async_copy(x_hbm.at[:, block(first)], x_ref.at[:, pl.ds(bs, bs)], local_sem.at[1])
    load_x2 = pltpu.make_async_copy(x_hbm.at[:, block(last)], x_ref.at[:, pl.ds(2 * bs, bs)], local_sem.at[2])
    load_b = pltpu.make_async_copy(b_hbm, b_ref, local_sem.at[3])
    load_bh = pltpu.make_async_copy(b_hbm.at[:, block(last)], bh_ref, local_sem.at[4])
    load_noise = pltpu.make_async_copy(noise_hbm.at[:, mine], noise_ref, local_sem.at[5])
    load_x0.start()
    load_b.start()
    load_x1.start()
    load_noise.start()

    @pl.when(jnp.logical_not(edge))
    def _():
        load_x2.start()
        load_bh.start()

    row = lax.broadcasted_iota(jnp.int32, (8, 128), 0)
    flags = jnp.zeros((8, 128), jnp.float32)
    for k in range(CHIPS):
        left = g * CHIPS + k
        listed = jnp.float32(0.0)
        for s in range(2):
            hit = (pairs_ref[s, 0] == left) & (pairs_ref[s, 1] == left + 1)
            listed = listed + jnp.where(hit, 1.0, 0.0)
        flags = jnp.where(row == k, listed, flags)
    flag_ref[me] = flags

    scale = inv_ref[...] * (W / 16.0)
    scale = jnp.broadcast_to(jnp.concatenate([scale, scale], 1), (128, 2 * F)).T[0:F]
    inv = jnp.tile(scale, (1, ch // 128))

    def prepare(slot):
        def part(i, _):
            at = pl.ds(pl.multiple_of(slot * bs + i * ch, ch), ch)
            a, c = left_terms(x_ref[:, at], inv)
            l_ref[at, 0:128] = a
            l_ref[at, 128:256] = a
            l_ref[at, 256:384] = a
            l_ref[at, 384:512] = c
            return 0

        lax.fori_loop(0, bs // ch, part, 0)

    load_x0.wait()
    prepare(0)
    for i in range(own // ch):
        at = pl.ds(pl.multiple_of(h * own + i * ch, ch), ch)
        r_ref[:, i * ch : (i + 1) * ch] = right_terms(x_ref[:, at], inv)
    load_b.wait()
    v_ref[0:R, 0:bs] = b_ref[:, block(y)].astype(jnp.bfloat16)
    v_ref[0:R, bs : 2 * bs] = b_ref[:, block(first)].astype(jnp.bfloat16)

    pl.semaphore_wait(barrier, 5 + nx + nz + jnp.where(edge, 1, 0))

    half = pl.ds(pl.multiple_of(h * own, own), own)
    half_x = pl.ds(pl.multiple_of(2 * bs + h * own, own), own)
    other = pl.ds(pl.multiple_of((1 - h) * own, own), own)
    other_x = pl.ds(pl.multiple_of(2 * bs + (1 - h) * own, own), own)

    def halo_x(device):
        return pltpu.make_async_remote_copy(
            x_ref.at[:, half], x_ref.at[:, half_x], halo_send.at[0], halo_recv.at[h],
            device_id=device, device_id_type=MESH)

    def halo_b(device):
        return pltpu.make_async_remote_copy(
            b_ref.at[:, mine], bh_ref.at[:, half], halo_send.at[1], halo_recv.at[2 + h],
            device_id=device, device_id_type=MESH)

    chunks = own // LANES

    def slab(i, c):
        return pl.ds(pl.multiple_of(i * own + c * LANES, LANES), LANES)

    def edge_q(device, c):
        return pltpu.make_async_remote_copy(
            q1_ref.at[:, slab(me, c)], qh_ref.at[:, slab(h, c)], edge_send.at[0, c], edge_recv.at[h, c],
            device_id=device, device_id_type=MESH)

    def edge_on(side, c):
        return pltpu.make_async_remote_copy(
            qh_ref.at[:, slab(side, c)], qh_ref.at[:, slab(side, c)], edge_send.at[1, c], edge_recv.at[side, c],
            device_id=partner, device_id_type=MESH)

    def pass_on(ref, at, k, sem):
        return pltpu.make_async_remote_copy(
            ref.at[:, at], ref.at[:, at], halo_send.at[2 + k], halo_recv.at[2 * k + sem],
            device_id=partner, device_id_type=MESH)

    forward_dev = (after, h)
    backward_dev = (before, (CHIPS - 1) * 2 + h)

    @pl.when(y == CHIPS - 1)
    def _():
        halo_x(forward_dev).start()
        halo_b(forward_dev).start()

    @pl.when(y == 0)
    def _():
        halo_x(backward_dev).start()
        halo_b(backward_dev).start()

    def flag_copy(k):
        return pltpu.make_async_remote_copy(
            flag_ref.at[me], flag_ref.at[me], flag_send.at[k], flag_recv.at[k],
            device_id=(g, (me + k) % 8), device_id_type=MESH)

    def flag_arrival(k):
        src = (me + 8 - k) % 8
        return pltpu.make_async_remote_copy(
            flag_ref.at[src], flag_ref.at[src], flag_send.at[k], flag_recv.at[k],
            device_id=(g, src), device_id_type=MESH)

    for k in range(1, 8):
        flag_copy(k).start()
    load_x1.wait()
    prepare(1)

    sig = sig_ref[0]
    passes = functools.partial(
        tile_pass, l_ref=l_ref, r_ref=r_ref, k_ref=k_ref, v_ref=v_ref, p_ref=p_ref, s_ref=s_ref,
        sig=sig, sq_ref=sq_ref, h_ref=h_ref)

    passes(0, ch, bs)

    for k in range(1, 8):
        flag_arrival(k).wait_recv()
    total_flags = flag_ref[0]
    for k in range(1, 8):
        total_flags = total_flags + flag_ref[k]
    group_ref[0] = total_flags
    group_copy = pltpu.make_async_remote_copy(
        group_ref.at[0], group_ref.at[1], flag_send.at[0], flag_recv.at[0],
        device_id=forward_dev, device_id_type=MESH)

    @pl.when(y == CHIPS - 1)
    def _():
        group_copy.start()

    passes(1, ch, bs)

    @pl.when(jnp.logical_not(edge))
    def _():
        load_x2.wait()

    @pl.when(edge)
    def _():
        pass_on(x_ref, half_x, 0, h).wait_recv()
        pass_on(x_ref, half_x, 0, h).start()
        pass_on(x_ref, other_x, 0, 1 - h).wait_recv()

    prepare(2)
    passes(2, ch, bs, multiply=False)

    @pl.when(jnp.logical_not(edge))
    def _():
        load_bh.wait()

    @pl.when(edge)
    def _():
        pass_on(bh_ref, half, 1, h).wait_recv()
        pass_on(bh_ref, half, 1, h).start()
        pass_on(bh_ref, other, 1, 1 - h).wait_recv()

    v_ref[0:R, 2 * bs : 3 * bs] = bh_ref[...].astype(jnp.bfloat16)
    load_noise.wait()

    @pl.when(y == 0)
    def _():
        group_copy.wait_recv()
        group_ref[2, 0:1, :] = group_ref[1, CHIPS - 1 : CHIPS, :]

    @pl.when(y > 0)
    def _():
        group_ref[2, 0:1, :] = group_ref[0, pl.ds(y, 1), :]

    flag_first = jnp.tile(group_ref[0, pl.ds(jnp.maximum(y - 1, 0), 1), :], (1, LANES // 128))
    flag_last = jnp.tile(group_ref[2, 0:1, :], (1, LANES // 128))

    to_up, to_down = (g, up * 2 + h), (g, down * 2 + h)

    def part_copy(t, ref, which, c, k, device):
        return pltpu.make_async_remote_copy(
            ref.at[:, slab(which, c)], ref.at[:, slab(which, c)], part_send.at[t, k, c], part_recv.at[t, which, c],
            device_id=device, device_id_type=MESH)

    def hand_out(t, ref, c):
        part_copy(t, ref, me, c, 0, to_up).start()
        part_copy(t, ref, me, c, 1, to_down).start()
        part_copy(t, ref, me, c, 2, partner).start()

    def image(cols, vec):
        return diag_ref[:, cols] * vec + (p_ref[0, :, cols] + flag_first * p_ref[1, :, cols] + flag_last * p_ref[2, :, cols])

    def first_image(j, _):
        cols = pl.ds(pl.multiple_of(j * LANES, LANES), LANES)
        at = slab(me, j)
        rows = pl.ds(2 * bs, bs)
        p_ref[2, :, cols] = jnp.dot(v_ref[0:R, rows], k_ref[rows, cols], preferred_element_type=jnp.float32)
        diag_ref[:, cols] = noise_ref[:, cols] + flag_first * s_ref[1, 0:1, cols] + flag_last * s_ref[2, 0:1, cols]
        q1_ref[:, at] = image(cols, b_ref[:, at])
        hand_out(0, q1_ref, j)

        @pl.when(y == CHIPS - 1)
        def _():
            edge_q(forward_dev, j).start()

        @pl.when(y == 0)
        def _():
            edge_q(backward_dev, j).start()

        return 0

    lax.fori_loop(0, chunks, first_image, 0)

    lane = lax.broadcasted_iota(jnp.int32, (R, 128), 1)

    def set_stats(t, arrays):
        stats = jnp.zeros((R, 128), jnp.float32)
        for k, a in enumerate(arrays):
            stats = jnp.where(lane == k, jnp.sum(a, axis=1, keepdims=True), stats)
        padded = jnp.concatenate([stats, jnp.zeros((128 - R, 128), jnp.float32)], 0)
        st_ref[t, me] = padded.T[0:8]

    def sum_copies(t, ref, stage, n, place, device_of):
        def send(k):
            return pltpu.make_async_remote_copy(
                ref.at[t, place], ref.at[t, place], sum_send.at[t, stage, k], sum_recv.at[t, stage, k],
                device_id=device_of((place + k) % n), device_id_type=MESH)

        def arrival(k):
            src = (place + n - k) % n
            return pltpu.make_async_remote_copy(
                ref.at[t, src], ref.at[t, src], sum_send.at[t, stage, k], sum_recv.at[t, stage, k],
                device_id=device_of(src), device_id_type=MESH)

        def start():
            for k in range(1, n):
                send(k).start()

        def finish():
            for k in range(1, n):
                arrival(k).wait_recv()
            total = ref[t, 0]
            for k in range(1, n):
                total = total + ref[t, k]
            return total

        def drain():
            for k in range(1, n):
                send(k).wait_send()

        return start, finish, drain

    def stages(t):
        return (
            sum_copies(t, st_ref, 0, 8, me, lambda p: (g, p)),
            sum_copies(t, sx_ref, 1, nx, gx, lambda p: (p * nz + gz, me)),
            sum_copies(t, sz_ref, 2, nz, gz, lambda p: (gx * nz + p, me)),
        )

    def own_chip(t):
        for c in range(chunks):
            ref = (q1_ref, q2_ref)[t]
            part_copy(t, ref, y * 2 + 1 - h, c, 0, partner).wait_recv()

    def parts(t, ref):
        def arrived(which, c):
            part_copy(t, ref, which, c, 0, partner).wait_recv()

        def relay():
            for c in range(chunks):
                arrived(down * 2 + h, c)

                @pl.when(h == 0)
                def _():
                    part_copy(t, ref, down * 2 + h, c, 6, to_up).start()

                part_copy(t, ref, down * 2 + h, c, 3, partner).start()
                arrived(up * 2 + h, c)

                @pl.when(h == 1)
                def _():
                    part_copy(t, ref, up * 2 + h, c, 6, to_down).start()

                part_copy(t, ref, up * 2 + h, c, 4, partner).start()

        def near():
            for c in range(chunks):
                arrived(down * 2 + 1 - h, c)
                arrived(up * 2 + 1 - h, c)

        def far_on():
            for c in range(chunks):
                arrived(across * 2 + h, c)
                part_copy(t, ref, across * 2 + h, c, 5, partner).start()

        def far():
            for c in range(chunks):
                arrived(across * 2 + 1 - h, c)

        def drain():
            for c in range(chunks):
                for k in range(7):
                    part_copy(t, ref, me, c, k, partner).wait_send()

        return relay, near, far_on, far, drain

    relay, near, far_on, far, drain = parts(0, q1_ref)
    relay2, near2, far_on2, far2, drain2 = parts(1, q2_ref)
    (a_start, a_finish, a_drain), (x_start, x_finish, x_drain), (z_start, z_finish, z_drain) = stages(0)

    def two_terms(slot, q):
        at = pl.ds(slot * bs, bs)
        hi = q.astype(jnp.bfloat16)
        v_ref[0:R, at] = hi
        v_ref[R : 2 * R, at] = (q - hi.astype(jnp.float32)).astype(jnp.bfloat16)

    def product(slot, cols):
        rows = pl.ds(slot * bs, bs)
        both = jnp.dot(v_ref[:, rows], k_ref[rows, cols], preferred_element_type=jnp.float32)
        return both[0:R] + both[R : 2 * R]

    own_chip(0)
    two_terms(0, q1_ref[:, block(y)])

    def own_lanes(j, _):
        cols = pl.ds(pl.multiple_of(j * LANES, LANES), LANES)
        p_ref[0, :, cols] = product(0, cols)
        return 0

    lax.fori_loop(0, chunks, own_lanes, 0)
    relay()

    @pl.when(edge)
    def _():
        for c in range(chunks):
            edge_on(h, c).wait_recv()
            edge_on(h, c).start()

    near()

    @pl.when(edge)
    def _():
        for c in range(chunks):
            edge_on(1 - h, c).wait_recv()

    @pl.when(jnp.logical_not(edge))
    def _():
        qh_ref[...] = q1_ref[:, block(last)]

    two_terms(1, q1_ref[:, block(first)])
    two_terms(2, qh_ref[...])

    def second_image(j, _):
        cols = pl.ds(pl.multiple_of(j * LANES, LANES), LANES)
        p_ref[1, :, cols] = product(1, cols)
        p_ref[2, :, cols] = product(2, cols)
        at = slab(me, j)
        q2_ref[:, at] = image(cols, q1_ref[:, at])
        hand_out(1, q2_ref, j)
        return 0

    lax.fori_loop(0, chunks, second_image, 0)
    b_own, q_own, w_own = b_ref[:, mine], q1_ref[:, mine], q2_ref[:, mine]
    set_stats(0, (b_own * b_own, b_own * q_own, q_own * q_own, b_own * w_own, q_own * w_own))
    a_start()
    far_on()
    sx_ref[0, gx] = a_finish()
    x_start()
    relay2()
    sz_ref[0, gz] = x_finish()
    z_start()
    far()
    q1_out = pltpu.make_async_copy(q1_ref, q1_hbm, out_sem.at[0])
    q1_out.start()
    far_on2()
    own_chip(1)
    near2()
    far2()
    q2_out = pltpu.make_async_copy(q2_ref, q2_hbm, out_sem.at[1])
    q2_out.start()
    total = z_finish()
    norm, curve, square, cross, cube = [total[k : k + 1] for k in range(5)]
    step1 = norm / curve
    norm2 = norm - 2.0 * step1 * curve + step1 * step1 * square
    ratio = norm2 / norm
    grown = 1.0 + ratio
    curve2 = grown * (grown * curve - step1 * (square + cross)) + step1 * step1 * cube
    step2 = norm2 / curve2
    stacked = jnp.zeros((8, 128), jnp.float32)
    for k, a in enumerate((step1, ratio, step2)):
        stacked = jnp.where(row == k, a, stacked)
    coef_ref[...] = jnp.concatenate([stacked, jnp.zeros((120, 128), jnp.float32)], 0).T[0:R]

    for k in range(1, 8):
        flag_copy(k).wait_send()
    for wait in (a_drain, x_drain, z_drain, drain, drain2):
        wait()

    @pl.when(edge)
    def _():
        halo_x(forward_dev).wait_send()
        halo_b(forward_dev).wait_send()
        pass_on(x_ref, half_x, 0, h).wait_send()
        pass_on(bh_ref, half, 1, h).wait_send()
        for c in range(chunks):
            edge_q(forward_dev, c).wait_send()
            edge_on(h, c).wait_send()

    @pl.when(y == CHIPS - 1)
    def _():
        group_copy.wait_send()

    q1_out.wait()
    q2_out.wait()


def body(features, inv_scale, signal, noise_var, right_side, block_pairs):
    local = features.shape[1]
    bs = local // CHIPS
    own = bs // 2
    nx, nz = TORUS[lax.axis_size("blk")]
    vmem = pltpu.VMEM
    dma = pltpu.SemaphoreType.DMA
    f32, bf16 = jnp.float32, jnp.bfloat16
    hbm = pl.BlockSpec(memory_space=pl.ANY)
    smem = pl.BlockSpec(memory_space=pltpu.SMEM)
    shape = jax.ShapeDtypeStruct(right_side.shape, f32)
    q1, q2, coef = pl.pallas_call(
        functools.partial(kernel, nx, nz, bs),
        name="conjugate_gradients",
        out_shape=(shape, shape, jax.ShapeDtypeStruct((R, 128), f32)),
        in_specs=[hbm, pl.BlockSpec(memory_space=pltpu.VMEM), smem, hbm, hbm, smem],
        out_specs=(hbm, hbm, pl.BlockSpec(memory_space=pltpu.VMEM)),
        scratch_shapes=[
            vmem((F, 3 * bs), f32),
            vmem((3 * bs, TERMS), bf16),
            vmem((TERMS, own), bf16),
            vmem((3 * bs, own), bf16),
            vmem((R, local), f32),
            vmem((R, bs), f32),
            vmem((R, local), f32),
            vmem((R, bs), f32),
            vmem((R, local), f32),
            vmem((2 * R, 3 * bs), bf16),
            vmem((3, R, own), f32),
            vmem((3, 8, own), f32),
            vmem((1, own), f32),
            vmem((2, bs // 4, LANES), f32),
            vmem((2, bs // 4, LANES), bf16),
            vmem((8, 8, 128), f32),
            vmem((3, 8, 128), f32),
            vmem((1, 8, 8, 128), f32),
            vmem((1, nx, 8, 128), f32),
            vmem((1, nz, 8, 128), f32),
            vmem((1, own), f32),
            dma((6,)),
            dma((2,)),
            dma((4,)),
            dma((4,)),
            dma((2, own // LANES)),
            dma((2, own // LANES)),
            dma((8,)),
            dma((8,)),
            dma((1, 3, 8)),
            dma((1, 3, 8)),
            dma((2, 7, own // LANES)),
            dma((2, 8, own // LANES)),
        ],
        compiler_params=pltpu.CompilerParams(
            collective_id=0, has_side_effects=True, vmem_limit_bytes=60 * 1024 * 1024
        ),
    )(features, inv_scale.reshape(1, -1), signal, noise_var.reshape(1, -1), right_side, block_pairs)
    step1, ratio, step2 = coef[:, 0:1], coef[:, 1:2], coef[:, 2:3]
    residual = right_side - step1 * q1
    image = (1.0 + ratio) * q1 - step1 * q2
    return step1 * right_side + step2 * (residual + ratio * right_side), residual - step2 * image


def solution(mesh):
    placed = (P(None, "blk"), P(), P(), P("blk"), P(None, "blk"), P(("blk", "pair"), None))
    return jax.shard_map(
        body,
        mesh=mesh,
        in_specs=placed,
        out_specs=(P(None, "blk"), P(None, "blk")),
        check_vma=False,
    )
```

```python
import functools
import math

import jax
import jax.numpy as jnp
from jax import lax
from jax.experimental import pallas as pl
from jax.experimental.pallas import tpu as pltpu
from jax.sharding import PartitionSpec as P

F = 64
R = 32
CHIPS = 4
TORUS = {32: (4, 8), 8: (2, 4), 2: (1, 2)}
LANES = 256
TERMS = 512
MESH = pl.DeviceIdType.MESH

ROOT3 = math.sqrt(3.0)
W = 2.0 * ROOT3 * math.log2(math.e)
SCALE = 2.0**-W / W**4
Q0 = 5.0 * (1.0 + 2.0 * ROOT3) * SCALE
Q1 = -(4.0 * (1.0 + 2.0 * ROOT3) + 10.0 * ROOT3) / W * SCALE
Q2 = 8.0 * ROOT3 / W**2 * SCALE
TINY = 1e-30


def split3(s):
    hi = s.astype(jnp.bfloat16)
    rest = s - hi.astype(jnp.float32)
    mid = rest.astype(jnp.bfloat16)
    lo = (rest - mid.astype(jnp.float32)).astype(jnp.bfloat16)
    return hi, mid, lo


def norm_rows(norms, first):
    n = norms.shape[1]
    hi, mid, lo = split3(norms)
    row = lax.broadcasted_iota(jnp.int32, (8, n), 0)
    base = 0 if first else 3
    ones = (row >= 3 - base) & (row < 6 - base)
    top = jnp.where(row == base, hi.astype(jnp.float32), 0.0)
    top = jnp.where(row == base + 1, mid.astype(jnp.float32), top)
    top = jnp.where(row == base + 2, lo.astype(jnp.float32), top)
    top = jnp.where(ones, 1.0, top)
    return jnp.concatenate([top, jnp.zeros((F - 8, n), jnp.float32)], 0).astype(jnp.bfloat16)


def left_terms(x, inv):
    s = x * inv
    norms = jnp.sum(s * s, axis=0, keepdims=True)
    hi, mid, lo = split3(-2.0 * s)
    return jnp.concatenate([hi, mid], 0).T, jnp.concatenate([lo, norm_rows(norms, False)], 0).T


def right_terms(x, inv):
    s = x * inv
    norms = jnp.sum(s * s, axis=0, keepdims=True)
    hi, mid, lo = split3(s)
    return jnp.concatenate([hi, hi, mid, mid, lo, jnp.zeros_like(lo), hi, norm_rows(norms, True)], 0)


def tile_values(sq, c0, c1, c2):
    y = jnp.maximum(sq, TINY)
    w = y * lax.rsqrt(y)
    u = jnp.maximum(W - w, 0.0)
    u2 = u * u
    return ((c2 * u + c1) * u + c0) * jnp.exp2(u) * (u2 * u2)


def tile_pass(slot, ch, bs, l_ref, r_ref, k_ref, v_ref, p_ref, s_ref, sig, sq_ref, h_ref, after=None):
    c0, c1, c2 = sig * Q0, sig * Q1, sig * Q2
    n = bs // ch
    base = slot * bs

    def lanes(j, _):
        cols = pl.ds(pl.multiple_of(j * LANES, LANES), LANES)

        def at(i):
            return pl.ds(pl.multiple_of(base + i * ch, ch), ch)

        def cross(i, buf):
            sq_ref[buf] = jnp.dot(l_ref[at(i), :], r_ref[:, cols], preferred_element_type=jnp.float32)

        def values(i, buf, sums):
            t = tile_values(sq_ref[buf], c0, c1, c2)
            half = t.astype(jnp.bfloat16)
            k_ref[at(i), cols] = half
            h_ref[buf] = half
            if slot == 0:
                return sums
            return sums + jnp.sum(t.reshape(ch // 8, 8, LANES), axis=0)

        def prod(i, buf, acc):
            return acc + jnp.dot(v_ref[0:R, at(i)], h_ref[buf], preferred_element_type=jnp.float32)

        acc = jnp.zeros((R, LANES), jnp.float32)
        sums = jnp.zeros((8, LANES), jnp.float32)
        cross(0, 0)
        cross(1, 1)
        sums = values(0, 0, sums)

        def rows(m, carry):
            acc, sums = carry
            i = 2 * m + 1
            cross(i + 1, 0)
            sums = values(i, 1, sums)
            acc = prod(i - 1, 0, acc)
            cross(i + 2, 1)
            sums = values(i + 1, 0, sums)
            acc = prod(i, 1, acc)
            return acc, sums

        acc, sums = lax.fori_loop(0, (n - 2) // 2, rows, (acc, sums))
        sums = values(n - 1, 1, sums)
        acc = prod(n - 2, 0, acc)
        acc = prod(n - 1, 1, acc)
        p_ref[slot, :, cols] = acc
        s_ref[slot, :, cols] = jnp.broadcast_to(jnp.sum(sums, axis=0, keepdims=True), (8, LANES))
        if after is not None:
            after(j, cols)
        return 0

    lax.fori_loop(0, p_ref.shape[2] // LANES, lanes, 0)


def kernel(
    nx, nz, bs,
    x_hbm, inv_ref, sig_ref, noise_hbm, b_hbm, pairs_ref,
    q1_hbm, q2_hbm, coef_ref,
    x_ref, l_ref, r_ref, k_ref, b_ref, bh_ref, q1_ref, qh_ref, q2_ref, v_ref,
    p_ref, s_ref, noise_ref, sq_ref, h_ref, flag_ref, group_ref, st_ref, sx_ref, sz_ref,
    diag_ref,
    local_sem, out_sem, halo_send, halo_recv, edge_send, edge_recv, flag_send, flag_recv, sum_send, sum_recv, part_send, part_recv,
):
    own = bs // 2
    ch = bs // 4
    count = nx * nz
    g = lax.axis_index("blk")
    me = lax.axis_index("pair")
    y, h = me // 2, me % 2
    gx, gz = g // nz, g % nz
    up, down, across = (y + 1) % CHIPS, (y + CHIPS - 1) % CHIPS, (y + 2) % CHIPS
    partner = (g, y * 2 + 1 - h)
    after, before = (g + 1) % count, (g + count - 1) % count
    edge = (y == 0) | (y == CHIPS - 1)
    first = jnp.where(y == 0, 1, y - 1)
    last = jnp.minimum(y + 1, CHIPS - 1)

    def block(i):
        return pl.ds(pl.multiple_of(i * bs, bs), bs)

    def piece(i):
        return pl.ds(pl.multiple_of(i * own, own), own)

    mine = piece(me)

    barrier = pltpu.get_barrier_semaphore()

    def greet(device):
        pl.semaphore_signal(barrier, inc=1, device_id=device, device_id_type=MESH)

    for k in range(1, 8):
        greet((g, (me + k) % 8))
    for k in range(1, nx):
        greet((((gx + k) % nx) * nz + gz, me))
    for k in range(1, nz):
        greet((gx * nz + (gz + k) % nz, me))

    top = y == CHIPS - 1
    crossing = (jnp.where(top, after, before), jnp.where(top, h, (CHIPS - 1) * 2 + h))
    beside = (jnp.where(top, before, after), me)
    beside_block = jnp.where(top, 0, CHIPS - 1)

    @pl.when(edge)
    def _():
        greet(crossing)
        greet((after, me))
        greet((before, me))

    load_x0 = pltpu.make_async_copy(x_hbm.at[:, block(y)], x_ref.at[:, pl.ds(0, bs)], local_sem.at[0])
    load_x1 = pltpu.make_async_copy(x_hbm.at[:, block(first)], x_ref.at[:, pl.ds(bs, bs)], local_sem.at[1])
    load_x2 = pltpu.make_async_copy(x_hbm.at[:, block(last)], x_ref.at[:, pl.ds(2 * bs, bs)], local_sem.at[2])
    load_b = pltpu.make_async_copy(b_hbm, b_ref, local_sem.at[3])
    load_bh = pltpu.make_async_copy(b_hbm.at[:, block(last)], bh_ref, local_sem.at[4])
    load_noise = pltpu.make_async_copy(noise_hbm.at[:, mine], noise_ref, local_sem.at[5])
    load_x0.start()
    load_b.start()
    load_x1.start()
    load_noise.start()

    @pl.when(jnp.logical_not(edge))
    def _():
        load_x2.start()
        load_bh.start()

    row = lax.broadcasted_iota(jnp.int32, (8, 128), 0)
    flags = jnp.zeros((8, 128), jnp.float32)
    for k in range(CHIPS):
        left = g * CHIPS + k
        listed = jnp.float32(0.0)
        for s in range(2):
            hit = (pairs_ref[s, 0] == left) & (pairs_ref[s, 1] == left + 1)
            listed = listed + jnp.where(hit, 1.0, 0.0)
        flags = jnp.where(row == k, listed, flags)
    flag_ref[me] = flags

    scale = inv_ref[...] * (W / 16.0)
    scale = jnp.broadcast_to(jnp.concatenate([scale, scale], 1), (128, 2 * F)).T[0:F]
    inv = jnp.tile(scale, (1, ch // 128))

    def prepare(slot):
        def part(i, _):
            at = pl.ds(pl.multiple_of(slot * bs + i * ch, ch), ch)
            a, c = left_terms(x_ref[:, at], inv)
            l_ref[at, 0:128] = a
            l_ref[at, 128:256] = a
            l_ref[at, 256:384] = a
            l_ref[at, 384:512] = c
            return 0

        lax.fori_loop(0, bs // ch, part, 0)

    load_x0.wait()
    prepare(0)
    for i in range(own // ch):
        at = pl.ds(pl.multiple_of(h * own + i * ch, ch), ch)
        r_ref[:, i * ch : (i + 1) * ch] = right_terms(x_ref[:, at], inv)
    load_b.wait()
    v_ref[0:R, 0:bs] = b_ref[:, block(y)].astype(jnp.bfloat16)
    v_ref[0:R, bs : 2 * bs] = b_ref[:, block(first)].astype(jnp.bfloat16)

    pl.semaphore_wait(barrier, 5 + nx + nz + jnp.where(edge, 3, 0))

    sub = own // 2

    def halo_at(base, side, k):
        return pl.ds(pl.multiple_of(base + side * own + k * sub, sub), sub)

    def halo(kind, k):
        ref, base = ((x_ref, 2 * bs), (bh_ref, 0))[kind]
        if kind == 0:
            src = x_ref.at[:, halo_at(0, h, 0)] if k == 0 else x_hbm.at[:, halo_at(beside_block * bs, h, 1)]
        else:
            src = b_ref.at[:, halo_at((y if k == 0 else beside_block) * bs, h, k)]
        return pltpu.make_async_remote_copy(
            src, ref.at[:, halo_at(base, h, k)], halo_send.at[2 * kind + k], halo_recv.at[kind, h, k],
            device_id=crossing if k == 0 else beside, device_id_type=MESH)

    def pass_on(kind, side, k):
        ref, base = ((x_ref, 2 * bs), (bh_ref, 0))[kind]
        at = halo_at(base, side, k)
        return pltpu.make_async_remote_copy(
            ref.at[:, at], ref.at[:, at], halo_send.at[4 + 2 * kind + k], halo_recv.at[kind, side, k],
            device_id=partner, device_id_type=MESH)

    def take_halo(kind):
        for k in range(2):
            pass_on(kind, h, k).wait_recv()
            pass_on(kind, h, k).start()
        for k in range(2):
            pass_on(kind, 1 - h, k).wait_recv()

    chunks = own // LANES

    def slab(i, c):
        return pl.ds(pl.multiple_of(i * own + c * LANES, LANES), LANES)

    def edge_q(device, c):
        return pltpu.make_async_remote_copy(
            q1_ref.at[:, slab(me, c)], qh_ref.at[:, slab(h, c)], edge_send.at[0, c], edge_recv.at[h, c],
            device_id=device, device_id_type=MESH)

    def edge_on(side, c):
        return pltpu.make_async_remote_copy(
            qh_ref.at[:, slab(side, c)], qh_ref.at[:, slab(side, c)], edge_send.at[1, c], edge_recv.at[side, c],
            device_id=partner, device_id_type=MESH)

    @pl.when(edge)
    def _():
        for kind in range(2):
            for k in range(2):
                halo(kind, k).start()

    def flag_copy(k):
        return pltpu.make_async_remote_copy(
            flag_ref.at[me], flag_ref.at[me], flag_send.at[k], flag_recv.at[k],
            device_id=(g, (me + k) % 8), device_id_type=MESH)

    def flag_arrival(k):
        src = (me + 8 - k) % 8
        return pltpu.make_async_remote_copy(
            flag_ref.at[src], flag_ref.at[src], flag_send.at[k], flag_recv.at[k],
            device_id=(g, src), device_id_type=MESH)

    for k in range(1, 8):
        flag_copy(k).start()
    load_x1.wait()
    prepare(1)

    sig = sig_ref[0]
    passes = functools.partial(
        tile_pass, l_ref=l_ref, r_ref=r_ref, k_ref=k_ref, v_ref=v_ref, p_ref=p_ref, s_ref=s_ref,
        sig=sig, sq_ref=sq_ref, h_ref=h_ref)

    passes(0, ch, bs)

    for k in range(1, 8):
        flag_arrival(k).wait_recv()
    total_flags = flag_ref[0]
    for k in range(1, 8):
        total_flags = total_flags + flag_ref[k]
    group_ref[0] = total_flags
    group_copy = pltpu.make_async_remote_copy(
        group_ref.at[0], group_ref.at[1], flag_send.at[0], flag_recv.at[0],
        device_id=crossing, device_id_type=MESH)

    @pl.when(y == CHIPS - 1)
    def _():
        group_copy.start()

    passes(1, ch, bs)

    @pl.when(jnp.logical_not(edge))
    def _():
        load_x2.wait()
        load_bh.wait()

    @pl.when(edge)
    def _():
        take_halo(0)

    prepare(2)

    @pl.when(edge)
    def _():
        take_halo(1)

    v_ref[0:R, 2 * bs : 3 * bs] = bh_ref[...].astype(jnp.bfloat16)
    load_noise.wait()

    @pl.when(y == 0)
    def _():
        group_copy.wait_recv()
        group_ref[2, 0:1, :] = group_ref[1, CHIPS - 1 : CHIPS, :]

    @pl.when(y > 0)
    def _():
        group_ref[2, 0:1, :] = group_ref[0, pl.ds(y, 1), :]

    flag_first = jnp.tile(group_ref[0, pl.ds(jnp.maximum(y - 1, 0), 1), :], (1, LANES // 128))
    flag_last = jnp.tile(group_ref[2, 0:1, :], (1, LANES // 128))

    to_up, to_down = (g, up * 2 + h), (g, down * 2 + h)

    def part_copy(t, ref, which, c, k, device):
        return pltpu.make_async_remote_copy(
            ref.at[:, slab(which, c)], ref.at[:, slab(which, c)], part_send.at[t, k, c], part_recv.at[t, which, c],
            device_id=device, device_id_type=MESH)

    def hand_out(t, ref, c):
        part_copy(t, ref, me, c, 0, to_up).start()
        part_copy(t, ref, me, c, 1, to_down).start()
        part_copy(t, ref, me, c, 2, partner).start()

    def image(cols, vec):
        return diag_ref[:, cols] * vec + (p_ref[0, :, cols] + flag_first * p_ref[1, :, cols] + flag_last * p_ref[2, :, cols])

    def first_image(j, cols):
        at = slab(me, j)
        diag_ref[:, cols] = noise_ref[:, cols] + flag_first * s_ref[1, 0:1, cols] + flag_last * s_ref[2, 0:1, cols]
        q1_ref[:, at] = image(cols, b_ref[:, at])
        hand_out(0, q1_ref, j)

        @pl.when(edge)
        def _():
            edge_q(crossing, j).start()

    passes(2, ch, bs, after=first_image)

    lane = lax.broadcasted_iota(jnp.int32, (R, 128), 1)

    def set_stats(t, arrays):
        stats = jnp.zeros((R, 128), jnp.float32)
        for k, a in enumerate(arrays):
            stats = jnp.where(lane == k, jnp.sum(a, axis=1, keepdims=True), stats)
        padded = jnp.concatenate([stats, jnp.zeros((128 - R, 128), jnp.float32)], 0)
        st_ref[t, me] = padded.T[0:8]

    def sum_copies(t, ref, stage, n, place, device_of):
        def send(k):
            return pltpu.make_async_remote_copy(
                ref.at[t, place], ref.at[t, place], sum_send.at[t, stage, k], sum_recv.at[t, stage, k],
                device_id=device_of((place + k) % n), device_id_type=MESH)

        def arrival(k):
            src = (place + n - k) % n
            return pltpu.make_async_remote_copy(
                ref.at[t, src], ref.at[t, src], sum_send.at[t, stage, k], sum_recv.at[t, stage, k],
                device_id=device_of(src), device_id_type=MESH)

        def start():
            for k in range(1, n):
                send(k).start()

        def finish():
            for k in range(1, n):
                arrival(k).wait_recv()
            total = ref[t, 0]
            for k in range(1, n):
                total = total + ref[t, k]
            return total

        def drain():
            for k in range(1, n):
                send(k).wait_send()

        return start, finish, drain

    def stages(t):
        return (
            sum_copies(t, st_ref, 0, 8, me, lambda p: (g, p)),
            sum_copies(t, sx_ref, 1, nx, gx, lambda p: (p * nz + gz, me)),
            sum_copies(t, sz_ref, 2, nz, gz, lambda p: (gx * nz + p, me)),
        )

    def own_chip(t):
        for c in range(chunks):
            ref = (q1_ref, q2_ref)[t]
            part_copy(t, ref, y * 2 + 1 - h, c, 0, partner).wait_recv()

    def parts(t, ref):
        def arrived(which, c):
            part_copy(t, ref, which, c, 0, partner).wait_recv()

        def relay():
            for c in range(chunks):
                arrived(down * 2 + h, c)

                @pl.when(h == 0)
                def _():
                    part_copy(t, ref, down * 2 + h, c, 6, to_up).start()

                part_copy(t, ref, down * 2 + h, c, 3, partner).start()
                arrived(up * 2 + h, c)

                @pl.when(h == 1)
                def _():
                    part_copy(t, ref, up * 2 + h, c, 6, to_down).start()

                part_copy(t, ref, up * 2 + h, c, 4, partner).start()

        def near():
            for c in range(chunks):
                arrived(down * 2 + 1 - h, c)
                arrived(up * 2 + 1 - h, c)

        def far_on():
            for c in range(chunks):
                arrived(across * 2 + h, c)
                part_copy(t, ref, across * 2 + h, c, 5, partner).start()

        def far():
            for c in range(chunks):
                arrived(across * 2 + 1 - h, c)

        def drain():
            for c in range(chunks):
                for k in range(7):
                    part_copy(t, ref, me, c, k, partner).wait_send()

        return relay, near, far_on, far, drain

    relay, near, far_on, far, drain = parts(0, q1_ref)
    relay2, near2, far_on2, far2, drain2 = parts(1, q2_ref)
    (a_start, a_finish, a_drain), (x_start, x_finish, x_drain), (z_start, z_finish, z_drain) = stages(0)

    def two_terms(slot, q):
        at = pl.ds(slot * bs, bs)
        hi = q.astype(jnp.bfloat16)
        v_ref[0:R, at] = hi
        v_ref[R : 2 * R, at] = (q - hi.astype(jnp.float32)).astype(jnp.bfloat16)

    def product(slot, cols):
        rows = pl.ds(slot * bs, bs)
        both = jnp.dot(v_ref[:, rows], k_ref[rows, cols], preferred_element_type=jnp.float32)
        return both[0:R] + both[R : 2 * R]

    own_chip(0)
    two_terms(0, q1_ref[:, block(y)])

    def own_lanes(j, _):
        cols = pl.ds(pl.multiple_of(j * LANES, LANES), LANES)
        p_ref[0, :, cols] = product(0, cols)
        return 0

    lax.fori_loop(0, chunks, own_lanes, 0)
    relay()

    @pl.when(edge)
    def _():
        for c in range(chunks):
            edge_on(h, c).wait_recv()
            edge_on(h, c).start()

    near()

    @pl.when(edge)
    def _():
        for c in range(chunks):
            edge_on(1 - h, c).wait_recv()

    @pl.when(jnp.logical_not(edge))
    def _():
        qh_ref[...] = q1_ref[:, block(last)]

    two_terms(1, q1_ref[:, block(first)])
    two_terms(2, qh_ref[...])

    def second_image(j, _):
        cols = pl.ds(pl.multiple_of(j * LANES, LANES), LANES)
        p_ref[1, :, cols] = product(1, cols)
        p_ref[2, :, cols] = product(2, cols)
        at = slab(me, j)
        q2_ref[:, at] = image(cols, q1_ref[:, at])
        hand_out(1, q2_ref, j)
        return 0

    lax.fori_loop(0, chunks, second_image, 0)
    b_own, q_own, w_own = b_ref[:, mine], q1_ref[:, mine], q2_ref[:, mine]
    set_stats(0, (b_own * b_own, b_own * q_own, q_own * q_own, b_own * w_own, q_own * w_own))
    a_start()
    far_on()
    sx_ref[0, gx] = a_finish()
    x_start()
    relay2()
    sz_ref[0, gz] = x_finish()
    z_start()
    far()
    q1_out = pltpu.make_async_copy(q1_ref, q1_hbm, out_sem.at[0])
    q1_out.start()
    far_on2()
    own_chip(1)
    near2()
    far2()
    q2_out = pltpu.make_async_copy(q2_ref, q2_hbm, out_sem.at[1])
    q2_out.start()
    total = z_finish()
    norm, curve, square, cross, cube = [total[k : k + 1] for k in range(5)]
    step1 = norm / curve
    norm2 = norm - 2.0 * step1 * curve + step1 * step1 * square
    ratio = norm2 / norm
    grown = 1.0 + ratio
    curve2 = grown * (grown * curve - step1 * (square + cross)) + step1 * step1 * cube
    step2 = norm2 / curve2
    stacked = jnp.zeros((8, 128), jnp.float32)
    for k, a in enumerate((step1, ratio, step2)):
        stacked = jnp.where(row == k, a, stacked)
    coef_ref[...] = jnp.concatenate([stacked, jnp.zeros((120, 128), jnp.float32)], 0).T[0:R]

    for k in range(1, 8):
        flag_copy(k).wait_send()
    for wait in (a_drain, x_drain, z_drain, drain, drain2):
        wait()

    @pl.when(edge)
    def _():
        for kind in range(2):
            for k in range(2):
                halo(kind, k).wait_send()
                pass_on(kind, h, k).wait_send()
        for c in range(chunks):
            edge_q(crossing, c).wait_send()
            edge_on(h, c).wait_send()

    @pl.when(y == CHIPS - 1)
    def _():
        group_copy.wait_send()

    q1_out.wait()
    q2_out.wait()


def combine(coef_ref, b_ref, q1_ref, q2_ref, sol_ref, res_ref):
    step1, ratio, step2 = coef_ref[:, 0:1], coef_ref[:, 1:2], coef_ref[:, 2:3]
    b, q1 = b_ref[...], q1_ref[...]
    residual = b - step1 * q1
    sol_ref[...] = step1 * b + step2 * (residual + ratio * b)
    res_ref[...] = residual - step2 * ((1.0 + ratio) * q1 - step1 * q2_ref[...])


def body(features, inv_scale, signal, noise_var, right_side, block_pairs):
    local = features.shape[1]
    bs = local // CHIPS
    own = bs // 2
    nx, nz = TORUS[lax.axis_size("blk")]
    vmem = pltpu.VMEM
    dma = pltpu.SemaphoreType.DMA
    f32, bf16 = jnp.float32, jnp.bfloat16
    hbm = pl.BlockSpec(memory_space=pl.ANY)
    smem = pl.BlockSpec(memory_space=pltpu.SMEM)
    shape = jax.ShapeDtypeStruct(right_side.shape, f32)
    q1, q2, coef = pl.pallas_call(
        functools.partial(kernel, nx, nz, bs),
        name="conjugate_gradients",
        out_shape=(shape, shape, jax.ShapeDtypeStruct((R, 128), f32)),
        in_specs=[hbm, pl.BlockSpec(memory_space=pltpu.VMEM), smem, hbm, hbm, smem],
        out_specs=(hbm, hbm, pl.BlockSpec(memory_space=pltpu.VMEM)),
        scratch_shapes=[
            vmem((F, 3 * bs), f32),
            vmem((3 * bs, TERMS), bf16),
            vmem((TERMS, own), bf16),
            vmem((3 * bs, own), bf16),
            vmem((R, local), f32),
            vmem((R, bs), f32),
            vmem((R, local), f32),
            vmem((R, bs), f32),
            vmem((R, local), f32),
            vmem((2 * R, 3 * bs), bf16),
            vmem((3, R, own), f32),
            vmem((3, 8, own), f32),
            vmem((1, own), f32),
            vmem((2, bs // 4, LANES), f32),
            vmem((2, bs // 4, LANES), bf16),
            vmem((8, 8, 128), f32),
            vmem((3, 8, 128), f32),
            vmem((1, 8, 8, 128), f32),
            vmem((1, nx, 8, 128), f32),
            vmem((1, nz, 8, 128), f32),
            vmem((1, own), f32),
            dma((6,)),
            dma((2,)),
            dma((8,)),
            dma((2, 2, 2)),
            dma((2, own // LANES)),
            dma((2, own // LANES)),
            dma((8,)),
            dma((8,)),
            dma((1, 3, 8)),
            dma((1, 3, 8)),
            dma((2, 7, own // LANES)),
            dma((2, 8, own // LANES)),
        ],
        compiler_params=pltpu.CompilerParams(
            collective_id=0, has_side_effects=True, vmem_limit_bytes=60 * 1024 * 1024
        ),
    )(features, inv_scale.reshape(1, -1), signal, noise_var.reshape(1, -1), right_side, block_pairs)
    blocks = pl.BlockSpec((R, bs), lambda i: (0, i))
    return pl.pallas_call(
        combine,
        name="combine",
        grid=(CHIPS,),
        out_shape=(shape, shape),
        in_specs=[pl.BlockSpec((R, 128), lambda i: (0, 0)), blocks, blocks, blocks],
        out_specs=(blocks, blocks),
    )(coef, right_side, q1, q2)


def solution(mesh):
    placed = (P(None, "blk"), P(), P(), P("blk"), P(None, "blk"), P(("blk", "pair"), None))
    return jax.shard_map(
        body,
        mesh=mesh,
        in_specs=placed,
        out_specs=(P(None, "blk"), P(None, "blk")),
        check_vma=False,
    )
```

```python
import functools
import math

import jax
import jax.numpy as jnp
from jax import lax
from jax.experimental import pallas as pl
from jax.experimental.pallas import tpu as pltpu
from jax.sharding import PartitionSpec as P

F = 64
R = 32
CHIPS = 4
TORUS = {32: (4, 8), 8: (2, 4), 2: (1, 2)}
LANES = 256
TERMS = 512
MESH = pl.DeviceIdType.MESH

ROOT3 = math.sqrt(3.0)
W = 2.0 * ROOT3 * math.log2(math.e)
SCALE = 2.0**-W / W**4
Q0 = 5.0 * (1.0 + 2.0 * ROOT3) * SCALE
Q1 = -(4.0 * (1.0 + 2.0 * ROOT3) + 10.0 * ROOT3) / W * SCALE
Q2 = 8.0 * ROOT3 / W**2 * SCALE
TINY = 1e-30


def split3(s):
    hi = s.astype(jnp.bfloat16)
    rest = s - hi.astype(jnp.float32)
    mid = rest.astype(jnp.bfloat16)
    lo = (rest - mid.astype(jnp.float32)).astype(jnp.bfloat16)
    return hi, mid, lo


def norm_rows(norms, first):
    n = norms.shape[1]
    hi, mid, lo = split3(norms)
    row = lax.broadcasted_iota(jnp.int32, (8, n), 0)
    base = 0 if first else 3
    ones = (row >= 3 - base) & (row < 6 - base)
    top = jnp.where(row == base, hi.astype(jnp.float32), 0.0)
    top = jnp.where(row == base + 1, mid.astype(jnp.float32), top)
    top = jnp.where(row == base + 2, lo.astype(jnp.float32), top)
    top = jnp.where(ones, 1.0, top)
    return jnp.concatenate([top, jnp.zeros((F - 8, n), jnp.float32)], 0).astype(jnp.bfloat16)


def left_terms(x, inv):
    s = x * inv
    norms = jnp.sum(s * s, axis=0, keepdims=True)
    hi, mid, lo = split3(-2.0 * s)
    return jnp.concatenate([hi, mid], 0).T, jnp.concatenate([lo, norm_rows(norms, False)], 0).T


def right_terms(x, inv):
    s = x * inv
    norms = jnp.sum(s * s, axis=0, keepdims=True)
    hi, mid, lo = split3(s)
    return jnp.concatenate([hi, hi, mid, mid, lo, jnp.zeros_like(lo), hi, norm_rows(norms, True)], 0)


def tile_values(sq, c0, c1, c2):
    y = jnp.maximum(sq, TINY)
    w = y * lax.rsqrt(y)
    u = jnp.maximum(W - w, 0.0)
    u2 = u * u
    return ((c2 * u + c1) * u + c0) * jnp.exp2(u) * (u2 * u2)


def tile_pass(slot, ch, bs, l_ref, r_ref, k_ref, v_ref, p_ref, s_ref, sig, sq_ref, h_ref, after=None):
    c0, c1, c2 = sig * Q0, sig * Q1, sig * Q2
    n = bs // ch
    base = slot * bs

    def lanes(j, _):
        cols = pl.ds(pl.multiple_of(j * LANES, LANES), LANES)

        def at(i):
            return pl.ds(pl.multiple_of(base + i * ch, ch), ch)

        def cross(i, buf):
            sq_ref[buf] = jnp.dot(l_ref[at(i), :], r_ref[:, cols], preferred_element_type=jnp.float32)

        def values(i, buf, sums):
            t = tile_values(sq_ref[buf], c0, c1, c2)
            half = t.astype(jnp.bfloat16)
            k_ref[at(i), cols] = half
            h_ref[buf] = half
            if slot == 0:
                return sums
            return sums + jnp.sum(t.reshape(ch // 8, 8, LANES), axis=0)

        def prod(i, buf, acc):
            return acc + jnp.dot(v_ref[0:R, at(i)], h_ref[buf], preferred_element_type=jnp.float32)

        acc = jnp.zeros((R, LANES), jnp.float32)
        sums = jnp.zeros((8, LANES), jnp.float32)
        cross(0, 0)
        cross(1, 1)
        sums = values(0, 0, sums)

        def rows(m, carry):
            acc, sums = carry
            i = 2 * m + 1
            cross(i + 1, 0)
            sums = values(i, 1, sums)
            acc = prod(i - 1, 0, acc)
            cross(i + 2, 1)
            sums = values(i + 1, 0, sums)
            acc = prod(i, 1, acc)
            return acc, sums

        acc, sums = lax.fori_loop(0, (n - 2) // 2, rows, (acc, sums))
        sums = values(n - 1, 1, sums)
        acc = prod(n - 2, 0, acc)
        acc = prod(n - 1, 1, acc)
        p_ref[slot, :, cols] = acc
        s_ref[slot, :, cols] = jnp.broadcast_to(jnp.sum(sums, axis=0, keepdims=True), (8, LANES))
        if after is not None:
            after(j, cols)
        return 0

    lax.fori_loop(0, p_ref.shape[2] // LANES, lanes, 0)


def kernel(
    nx, nz, bs,
    x_hbm, inv_ref, sig_ref, noise_hbm, b_hbm, pairs_ref,
    q1_out, q2_out, coef_ref,
    x_ref, l_ref, r_ref, k_ref, b_ref, bh_ref, q1_ref, qh_ref, q2_ref, v_ref,
    p_ref, s_ref, noise_ref, sq_ref, h_ref, flag_ref, group_ref, st_ref, sx_ref, sz_ref,
    diag_ref,
    local_sem, halo_send, halo_recv, edge_send, edge_recv, flag_send, flag_recv, sum_send, sum_recv, part_send, part_recv,
):
    own = bs // 2
    ch = bs // 4
    count = nx * nz
    g = lax.axis_index("blk")
    me = lax.axis_index("pair")
    y, h = me // 2, me % 2
    gx, gz = g // nz, g % nz
    up, down, across = (y + 1) % CHIPS, (y + CHIPS - 1) % CHIPS, (y + 2) % CHIPS
    partner = (g, y * 2 + 1 - h)
    after, before = (g + 1) % count, (g + count - 1) % count
    edge = (y == 0) | (y == CHIPS - 1)
    first = jnp.where(y == 0, 1, y - 1)
    last = jnp.minimum(y + 1, CHIPS - 1)

    def block(i):
        return pl.ds(pl.multiple_of(i * bs, bs), bs)

    def piece(i):
        return pl.ds(pl.multiple_of(i * own, own), own)

    mine = piece(me)

    barrier = pltpu.get_barrier_semaphore()

    def greet(device):
        pl.semaphore_signal(barrier, inc=1, device_id=device, device_id_type=MESH)

    for k in range(1, 8):
        greet((g, (me + k) % 8))
    for k in range(1, nx):
        greet((((gx + k) % nx) * nz + gz, me))
    for k in range(1, nz):
        greet((gx * nz + (gz + k) % nz, me))

    top = y == CHIPS - 1
    crossing = (jnp.where(top, after, before), jnp.where(top, h, (CHIPS - 1) * 2 + h))
    beside = (jnp.where(top, before, after), me)
    beside_block = jnp.where(top, 0, CHIPS - 1)

    @pl.when(edge)
    def _():
        greet(crossing)
        greet((after, me))
        greet((before, me))

    load_x0 = pltpu.make_async_copy(x_hbm.at[:, block(y)], x_ref.at[:, pl.ds(0, bs)], local_sem.at[0])
    load_x1 = pltpu.make_async_copy(x_hbm.at[:, block(first)], x_ref.at[:, pl.ds(bs, bs)], local_sem.at[1])
    load_x2 = pltpu.make_async_copy(x_hbm.at[:, block(last)], x_ref.at[:, pl.ds(2 * bs, bs)], local_sem.at[2])
    load_b = pltpu.make_async_copy(b_hbm, b_ref, local_sem.at[3])
    load_bh = pltpu.make_async_copy(b_hbm.at[:, block(last)], bh_ref, local_sem.at[4])
    load_noise = pltpu.make_async_copy(noise_hbm.at[:, mine], noise_ref, local_sem.at[5])
    load_x0.start()
    load_b.start()
    load_x1.start()
    load_noise.start()

    @pl.when(jnp.logical_not(edge))
    def _():
        load_x2.start()
        load_bh.start()

    row = lax.broadcasted_iota(jnp.int32, (8, 128), 0)
    flags = jnp.zeros((8, 128), jnp.float32)
    for k in range(CHIPS):
        left = g * CHIPS + k
        listed = jnp.float32(0.0)
        for s in range(2):
            hit = (pairs_ref[s, 0] == left) & (pairs_ref[s, 1] == left + 1)
            listed = listed + jnp.where(hit, 1.0, 0.0)
        flags = jnp.where(row == k, listed, flags)
    flag_ref[me] = flags

    scale = inv_ref[...] * (W / 16.0)
    scale = jnp.broadcast_to(jnp.concatenate([scale, scale], 1), (128, 2 * F)).T[0:F]
    inv = jnp.tile(scale, (1, ch // 128))

    def prepare(slot):
        def part(i, _):
            at = pl.ds(pl.multiple_of(slot * bs + i * ch, ch), ch)
            a, c = left_terms(x_ref[:, at], inv)
            l_ref[at, 0:128] = a
            l_ref[at, 128:256] = a
            l_ref[at, 256:384] = a
            l_ref[at, 384:512] = c
            return 0

        lax.fori_loop(0, bs // ch, part, 0)

    load_x0.wait()
    prepare(0)
    for i in range(own // ch):
        at = pl.ds(pl.multiple_of(h * own + i * ch, ch), ch)
        r_ref[:, i * ch : (i + 1) * ch] = right_terms(x_ref[:, at], inv)
    load_b.wait()
    v_ref[0:R, 0:bs] = b_ref[:, block(y)].astype(jnp.bfloat16)
    v_ref[0:R, bs : 2 * bs] = b_ref[:, block(first)].astype(jnp.bfloat16)

    pl.semaphore_wait(barrier, 5 + nx + nz + jnp.where(edge, 3, 0))

    sub = own // 2

    def halo_at(base, side, k):
        return pl.ds(pl.multiple_of(base + side * own + k * sub, sub), sub)

    def halo(kind, k):
        ref, base = ((x_ref, 2 * bs), (bh_ref, 0))[kind]
        if kind == 0:
            src = x_ref.at[:, halo_at(0, h, 0)] if k == 0 else x_hbm.at[:, halo_at(beside_block * bs, h, 1)]
        else:
            src = b_ref.at[:, halo_at((y if k == 0 else beside_block) * bs, h, k)]
        return pltpu.make_async_remote_copy(
            src, ref.at[:, halo_at(base, h, k)], halo_send.at[2 * kind + k], halo_recv.at[kind, h, k],
            device_id=crossing if k == 0 else beside, device_id_type=MESH)

    def pass_on(kind, side, k):
        ref, base = ((x_ref, 2 * bs), (bh_ref, 0))[kind]
        at = halo_at(base, side, k)
        return pltpu.make_async_remote_copy(
            ref.at[:, at], ref.at[:, at], halo_send.at[4 + 2 * kind + k], halo_recv.at[kind, side, k],
            device_id=partner, device_id_type=MESH)

    def take_halo(kind):
        for k in range(2):
            pass_on(kind, h, k).wait_recv()
            pass_on(kind, h, k).start()
        for k in range(2):
            pass_on(kind, 1 - h, k).wait_recv()

    chunks = own // LANES

    def slab(i, c):
        return pl.ds(pl.multiple_of(i * own + c * LANES, LANES), LANES)

    def edge_q(device, c):
        return pltpu.make_async_remote_copy(
            q1_ref.at[:, slab(me, c)], qh_ref.at[:, slab(h, c)], edge_send.at[0, c], edge_recv.at[h, c],
            device_id=device, device_id_type=MESH)

    def edge_on(side, c):
        return pltpu.make_async_remote_copy(
            qh_ref.at[:, slab(side, c)], qh_ref.at[:, slab(side, c)], edge_send.at[1, c], edge_recv.at[side, c],
            device_id=partner, device_id_type=MESH)

    @pl.when(edge)
    def _():
        for kind in range(2):
            for k in range(2):
                halo(kind, k).start()

    def flag_copy(k):
        return pltpu.make_async_remote_copy(
            flag_ref.at[me], flag_ref.at[me], flag_send.at[k], flag_recv.at[k],
            device_id=(g, (me + k) % 8), device_id_type=MESH)

    def flag_arrival(k):
        src = (me + 8 - k) % 8
        return pltpu.make_async_remote_copy(
            flag_ref.at[src], flag_ref.at[src], flag_send.at[k], flag_recv.at[k],
            device_id=(g, src), device_id_type=MESH)

    for k in range(1, 8):
        flag_copy(k).start()
    load_x1.wait()
    prepare(1)

    sig = sig_ref[0]
    passes = functools.partial(
        tile_pass, l_ref=l_ref, r_ref=r_ref, k_ref=k_ref, v_ref=v_ref, p_ref=p_ref, s_ref=s_ref,
        sig=sig, sq_ref=sq_ref, h_ref=h_ref)

    passes(0, ch, bs)

    for k in range(1, 8):
        flag_arrival(k).wait_recv()
    total_flags = flag_ref[0]
    for k in range(1, 8):
        total_flags = total_flags + flag_ref[k]
    group_ref[0] = total_flags
    group_copy = pltpu.make_async_remote_copy(
        group_ref.at[0], group_ref.at[1], flag_send.at[0], flag_recv.at[0],
        device_id=crossing, device_id_type=MESH)

    @pl.when(y == CHIPS - 1)
    def _():
        group_copy.start()

    passes(1, ch, bs)

    @pl.when(jnp.logical_not(edge))
    def _():
        load_x2.wait()
        load_bh.wait()

    @pl.when(edge)
    def _():
        take_halo(0)

    prepare(2)

    @pl.when(edge)
    def _():
        take_halo(1)

    v_ref[0:R, 2 * bs : 3 * bs] = bh_ref[...].astype(jnp.bfloat16)
    load_noise.wait()

    @pl.when(y == 0)
    def _():
        group_copy.wait_recv()
        group_ref[2, 0:1, :] = group_ref[1, CHIPS - 1 : CHIPS, :]

    @pl.when(y > 0)
    def _():
        group_ref[2, 0:1, :] = group_ref[0, pl.ds(y, 1), :]

    flag_first = jnp.tile(group_ref[0, pl.ds(jnp.maximum(y - 1, 0), 1), :], (1, LANES // 128))
    flag_last = jnp.tile(group_ref[2, 0:1, :], (1, LANES // 128))

    to_up, to_down = (g, up * 2 + h), (g, down * 2 + h)

    def part_copy(t, ref, which, c, k, device):
        return pltpu.make_async_remote_copy(
            ref.at[:, slab(which, c)], ref.at[:, slab(which, c)], part_send.at[t, k, c], part_recv.at[t, which, c],
            device_id=device, device_id_type=MESH)

    def hand_out(t, ref, c):
        part_copy(t, ref, me, c, 0, to_up).start()
        part_copy(t, ref, me, c, 1, to_down).start()
        part_copy(t, ref, me, c, 2, partner).start()

    def image(cols, vec):
        return diag_ref[:, cols] * vec + (p_ref[0, :, cols] + flag_first * p_ref[1, :, cols] + flag_last * p_ref[2, :, cols])

    def first_image(j, cols):
        at = slab(me, j)
        diag_ref[:, cols] = noise_ref[:, cols] + flag_first * s_ref[1, 0:1, cols] + flag_last * s_ref[2, 0:1, cols]
        q1_ref[:, at] = image(cols, b_ref[:, at])
        hand_out(0, q1_ref, j)

        @pl.when(edge)
        def _():
            edge_q(crossing, j).start()

    passes(2, ch, bs, after=first_image)

    lane = lax.broadcasted_iota(jnp.int32, (R, 128), 1)

    def set_stats(t, arrays):
        stats = jnp.zeros((R, 128), jnp.float32)
        for k, a in enumerate(arrays):
            stats = jnp.where(lane == k, jnp.sum(a, axis=1, keepdims=True), stats)
        padded = jnp.concatenate([stats, jnp.zeros((128 - R, 128), jnp.float32)], 0)
        st_ref[t, me] = padded.T[0:8]

    def sum_copies(t, ref, stage, n, place, device_of):
        def send(k):
            return pltpu.make_async_remote_copy(
                ref.at[t, place], ref.at[t, place], sum_send.at[t, stage, k], sum_recv.at[t, stage, k],
                device_id=device_of((place + k) % n), device_id_type=MESH)

        def arrival(k):
            src = (place + n - k) % n
            return pltpu.make_async_remote_copy(
                ref.at[t, src], ref.at[t, src], sum_send.at[t, stage, k], sum_recv.at[t, stage, k],
                device_id=device_of(src), device_id_type=MESH)

        def start():
            for k in range(1, n):
                send(k).start()

        def finish():
            for k in range(1, n):
                arrival(k).wait_recv()
            total = ref[t, 0]
            for k in range(1, n):
                total = total + ref[t, k]
            return total

        def drain():
            for k in range(1, n):
                send(k).wait_send()

        return start, finish, drain

    def stages(t):
        return (
            sum_copies(t, st_ref, 0, 8, me, lambda p: (g, p)),
            sum_copies(t, sx_ref, 1, nx, gx, lambda p: (p * nz + gz, me)),
            sum_copies(t, sz_ref, 2, nz, gz, lambda p: (gx * nz + p, me)),
        )

    def own_chip(t):
        for c in range(chunks):
            ref = (q1_ref, q2_ref)[t]
            part_copy(t, ref, y * 2 + 1 - h, c, 0, partner).wait_recv()

    def parts(t, ref):
        def arrived(which, c):
            part_copy(t, ref, which, c, 0, partner).wait_recv()

        def relay():
            for c in range(chunks):
                arrived(down * 2 + h, c)

                @pl.when(h == 0)
                def _():
                    part_copy(t, ref, down * 2 + h, c, 6, to_up).start()

                part_copy(t, ref, down * 2 + h, c, 3, partner).start()
                arrived(up * 2 + h, c)

                @pl.when(h == 1)
                def _():
                    part_copy(t, ref, up * 2 + h, c, 6, to_down).start()

                part_copy(t, ref, up * 2 + h, c, 4, partner).start()

        def near():
            for c in range(chunks):
                arrived(down * 2 + 1 - h, c)
                arrived(up * 2 + 1 - h, c)

        def far_on():
            for c in range(chunks):
                arrived(across * 2 + h, c)
                part_copy(t, ref, across * 2 + h, c, 5, partner).start()

        def far():
            for c in range(chunks):
                arrived(across * 2 + 1 - h, c)

        def drain():
            for c in range(chunks):
                for k in range(7):
                    part_copy(t, ref, me, c, k, partner).wait_send()

        return relay, near, far_on, far, drain

    relay, near, far_on, far, drain = parts(0, q1_ref)
    relay2, near2, far_on2, far2, drain2 = parts(1, q2_ref)
    (a_start, a_finish, a_drain), (x_start, x_finish, x_drain), (z_start, z_finish, z_drain) = stages(0)

    def two_terms(slot, q):
        at = pl.ds(slot * bs, bs)
        hi = q.astype(jnp.bfloat16)
        v_ref[0:R, at] = hi
        v_ref[R : 2 * R, at] = (q - hi.astype(jnp.float32)).astype(jnp.bfloat16)

    def product(slot, cols):
        rows = pl.ds(slot * bs, bs)
        both = jnp.dot(v_ref[:, rows], k_ref[rows, cols], preferred_element_type=jnp.float32)
        return both[0:R] + both[R : 2 * R]

    own_chip(0)
    two_terms(0, q1_ref[:, block(y)])

    def own_lanes(j, _):
        cols = pl.ds(pl.multiple_of(j * LANES, LANES), LANES)
        p_ref[0, :, cols] = product(0, cols)
        return 0

    lax.fori_loop(0, chunks, own_lanes, 0)
    relay()

    @pl.when(edge)
    def _():
        for c in range(chunks):
            edge_on(h, c).wait_recv()
            edge_on(h, c).start()

    near()

    @pl.when(edge)
    def _():
        for c in range(chunks):
            edge_on(1 - h, c).wait_recv()

    @pl.when(jnp.logical_not(edge))
    def _():
        qh_ref[...] = q1_ref[:, block(last)]

    two_terms(1, q1_ref[:, block(first)])
    two_terms(2, qh_ref[...])

    def second_image(j, _):
        cols = pl.ds(pl.multiple_of(j * LANES, LANES), LANES)
        p_ref[1, :, cols] = product(1, cols)
        p_ref[2, :, cols] = product(2, cols)
        at = slab(me, j)
        q2_ref[:, at] = image(cols, q1_ref[:, at])
        hand_out(1, q2_ref, j)
        return 0

    lax.fori_loop(0, chunks, second_image, 0)
    b_own, q_own, w_own = b_ref[:, mine], q1_ref[:, mine], q2_ref[:, mine]
    set_stats(0, (b_own * b_own, b_own * q_own, q_own * q_own, b_own * w_own, q_own * w_own))
    a_start()
    far_on()
    sx_ref[0, gx] = a_finish()
    x_start()
    relay2()
    sz_ref[0, gz] = x_finish()
    z_start()
    far()
    q1_out[...] = q1_ref[...]
    far_on2()
    own_chip(1)
    near2()
    far2()
    q2_out[...] = q2_ref[...]
    total = z_finish()
    norm, curve, square, cross, cube = [total[k : k + 1] for k in range(5)]
    step1 = norm / curve
    norm2 = norm - 2.0 * step1 * curve + step1 * step1 * square
    ratio = norm2 / norm
    grown = 1.0 + ratio
    curve2 = grown * (grown * curve - step1 * (square + cross)) + step1 * step1 * cube
    step2 = norm2 / curve2
    stacked = jnp.zeros((8, 128), jnp.float32)
    for k, a in enumerate((step1, ratio, step2)):
        stacked = jnp.where(row == k, a, stacked)
    coef_ref[...] = jnp.concatenate([stacked, jnp.zeros((120, 128), jnp.float32)], 0).T[0:R]

    for k in range(1, 8):
        flag_copy(k).wait_send()
    for wait in (a_drain, x_drain, z_drain, drain, drain2):
        wait()

    @pl.when(edge)
    def _():
        for kind in range(2):
            for k in range(2):
                halo(kind, k).wait_send()
                pass_on(kind, h, k).wait_send()
        for c in range(chunks):
            edge_q(crossing, c).wait_send()
            edge_on(h, c).wait_send()

    @pl.when(y == CHIPS - 1)
    def _():
        group_copy.wait_send()


def combine(bs, coef_ref, b_ref, q1_ref, q2_ref, sol_hbm, res_hbm, sol_ref, res_ref, sem):
    step1, ratio, step2 = coef_ref[:, 0:1], coef_ref[:, 1:2], coef_ref[:, 2:3]
    copies = []
    for i in range(CHIPS):
        at = pl.ds(i * bs, bs)
        b, q1 = b_ref[:, at], q1_ref[:, at]
        residual = b - step1 * q1
        sol_ref[:, at] = step1 * b + step2 * (residual + ratio * b)
        res_ref[:, at] = residual - step2 * ((1.0 + ratio) * q1 - step1 * q2_ref[:, at])
        copies.append(pltpu.make_async_copy(sol_ref.at[:, at], sol_hbm.at[:, at], sem.at[2 * i]))
        copies.append(pltpu.make_async_copy(res_ref.at[:, at], res_hbm.at[:, at], sem.at[2 * i + 1]))
        copies[-2].start()
        copies[-1].start()
    for copy in copies:
        copy.wait()


def body(features, inv_scale, signal, noise_var, right_side, block_pairs):
    local = features.shape[1]
    bs = local // CHIPS
    own = bs // 2
    nx, nz = TORUS[lax.axis_size("blk")]
    vmem = pltpu.VMEM
    dma = pltpu.SemaphoreType.DMA
    f32, bf16 = jnp.float32, jnp.bfloat16
    hbm = pl.BlockSpec(memory_space=pl.ANY)
    on_chip = pl.BlockSpec(memory_space=pltpu.VMEM)
    smem = pl.BlockSpec(memory_space=pltpu.SMEM)
    shape = jax.ShapeDtypeStruct(right_side.shape, f32)
    q1, q2, coef = pl.pallas_call(
        functools.partial(kernel, nx, nz, bs),
        name="conjugate_gradients",
        out_shape=(vmem(right_side.shape, f32), vmem(right_side.shape, f32), vmem((R, 128), f32)),
        in_specs=[hbm, pl.BlockSpec(memory_space=pltpu.VMEM), smem, hbm, hbm, smem],
        out_specs=(on_chip,) * 3,
        scratch_shapes=[
            vmem((F, 3 * bs), f32),
            vmem((3 * bs, TERMS), bf16),
            vmem((TERMS, own), bf16),
            vmem((3 * bs, own), bf16),
            vmem((R, local), f32),
            vmem((R, bs), f32),
            vmem((R, local), f32),
            vmem((R, bs), f32),
            vmem((R, local), f32),
            vmem((2 * R, 3 * bs), bf16),
            vmem((3, R, own), f32),
            vmem((3, 8, own), f32),
            vmem((1, own), f32),
            vmem((2, bs // 4, LANES), f32),
            vmem((2, bs // 4, LANES), bf16),
            vmem((8, 8, 128), f32),
            vmem((3, 8, 128), f32),
            vmem((1, 8, 8, 128), f32),
            vmem((1, nx, 8, 128), f32),
            vmem((1, nz, 8, 128), f32),
            vmem((1, own), f32),
            dma((6,)),
            dma((8,)),
            dma((2, 2, 2)),
            dma((2, own // LANES)),
            dma((2, own // LANES)),
            dma((8,)),
            dma((8,)),
            dma((1, 3, 8)),
            dma((1, 3, 8)),
            dma((2, 7, own // LANES)),
            dma((2, 8, own // LANES)),
        ],
        compiler_params=pltpu.CompilerParams(
            collective_id=0, has_side_effects=True, vmem_limit_bytes=60 * 1024 * 1024
        ),
    )(features, inv_scale.reshape(1, -1), signal, noise_var.reshape(1, -1), right_side, block_pairs)
    return pl.pallas_call(
        functools.partial(combine, bs),
        name="combine",
        out_shape=(shape, shape),
        in_specs=[on_chip] * 4,
        out_specs=(hbm, hbm),
        scratch_shapes=[vmem(right_side.shape, f32), vmem(right_side.shape, f32), dma((2 * CHIPS,))],
        compiler_params=pltpu.CompilerParams(vmem_limit_bytes=16 * 1024 * 1024),
    )(coef, right_side, q1, q2)


def solution(mesh):
    placed = (P(None, "blk"), P(), P(), P("blk"), P(None, "blk"), P(("blk", "pair"), None))
    return jax.shard_map(
        body,
        mesh=mesh,
        in_specs=placed,
        out_specs=(P(None, "blk"), P(None, "blk")),
        check_vma=False,
    )
```
